32 devices in a mesh: gx: 8 (over z, core), gy: 4 (over y, x).
Axes of the slice: x: 2, y: 2, z: 4, core: 2. Of those that a mesh axis runs over, the one named last changes fastest.
Arguments:
- density: float32 [256, 256, 256], P('gx', 'gy'), may hold values from 0.05 to 2
Outputs:
- potential: float32 [256, 256, 256], P('gx', 'gy')
- energy: float32 [], replicated
The draws below stay inside these ranges and needn't reach their ends.
All inputs are finite; a program needn't handle non-finite values.
Results may differ from the reference program's by a relative error of at most 0.00005.
Values sent between devices are 32-bit elements.
No kernel may reach another device: no remote copies, remote signals or barrier semaphores. Data moves between devices by JAX's collectives and lax.ppermute only.
A program may use at most 128 MiB of HBM per device.

```python
import math
import jax
import jax.numpy as jnp

NX = 256
NY = 256
NZ = 256


def block_scale(stream_key, dims, split, least, high):
    gain = 1.0
    for position, blocks in split:
        heights = jax.random.uniform(jax.random.fold_in(jax.random.fold_in(stream_key, 6), position), (blocks,), jnp.float32, least / len(split), high / len(split))
        gain = gain * jnp.repeat(jnp.exp(heights), dims[position] // blocks).reshape((-1,) + (1,) * (len(dims) - 1 - position))
    return gain


def setup_inputs(seed: int = 0) -> dict:
    streams_of = jax.random.split(jax.random.key(seed), 2)
    density = jnp.clip(jnp.exp(math.log(2.0) - 3.6888794 * jax.random.uniform(streams_of[0], (NX, NY, NZ), jnp.float32) ** block_scale(streams_of[0], (NX, NY, NZ), ((0, 8), (1, 4)), -0.2, 0.2)), 0.05, 2.0)
    return dict(density=density)


spacing = 1.0
pbe_kappa = 0.804
pbe_mu = 0.2195149727645171
pbe_beta = 0.06672455060314922
pbe_gamma = 0.031090690869654894
pw_coef = 0.0310907
pw_alpha = 0.2137
pw_first = 7.5957
pw_second = 3.5876
pw_third = 1.6382
pw_fourth = 0.49294

def xc_energy(electrons, grad_sq):
    k_fermi = jnp.cbrt(3.0 * math.pi ** 2 * electrons)
    exch_unif = -0.75 * k_fermi / math.pi
    s_square = grad_sq / (4.0 * k_fermi ** 2 * electrons ** 2)
    enhance = 1.0 + pbe_kappa - pbe_kappa / (1.0 + pbe_mu * s_square / pbe_kappa)
    wigner = jnp.cbrt(3.0 / (4.0 * math.pi * electrons))
    root_rs = jnp.sqrt(wigner)
    series = 2.0 * pw_coef * (pw_first * root_rs + pw_second * wigner + pw_third * wigner * root_rs + pw_fourth * wigner ** 2)
    corr_unif = -2.0 * pw_coef * (1.0 + pw_alpha * wigner) * jnp.log(1.0 + 1.0 / series)
    screen_sq = 4.0 * k_fermi / math.pi
    t_square = grad_sq / (4.0 * screen_sq * electrons ** 2)
    factor = pbe_beta / pbe_gamma / jnp.expm1(-corr_unif / pbe_gamma)
    scaled = factor * t_square
    gradient_term = pbe_gamma * jnp.log(1.0 + pbe_beta / pbe_gamma * t_square * (1.0 + scaled) / (1.0 + scaled + scaled ** 2))
    return electrons * (exch_unif * enhance + corr_unif + gradient_term)

def summed_energy(electrons, grad_sq):
    return jnp.sum(xc_energy(electrons, grad_sq))

def wavenum(count):
    index = jnp.arange(count, dtype=jnp.int32)
    signed = jnp.where(index < count // 2, index, index - count)
    signed = jnp.where(index == count // 2, 0, signed)
    return signed.astype(jnp.float32) * (2.0 * math.pi / (count * spacing))

def reference(density):
    spectrum = jnp.fft.fftn(density)
    waves = (wavenum(NX)[:, None, None], wavenum(NY)[None, :, None], wavenum(NZ)[None, None, :])
    gradients = [jnp.real(jnp.fft.ifftn(1j * wavevec * spectrum)) for wavevec in waves]
    grad_sq = gradients[0] ** 2 + gradients[1] ** 2 + gradients[2] ** 2
    energy_sum, partials = jax.value_and_grad(summed_energy, argnums=(0, 1))(density, grad_sq)
    d_dens, d_grad = partials
    flux_spec = 1j * waves[0] * jnp.fft.fftn(2.0 * d_grad * gradients[0])
    flux_spec = flux_spec + 1j * waves[1] * jnp.fft.fftn(2.0 * d_grad * gradients[1])
    flux_spec = flux_spec + 1j * waves[2] * jnp.fft.fftn(2.0 * d_grad * gradients[2])
    divergence = jnp.real(jnp.fft.ifftn(flux_spec))
    potential = d_dens - divergence
    energy = energy_sum / (NX * NY * NZ)
    return (potential, energy)
```

```python
import math

import jax
import jax.numpy as jnp
import numpy as np
from jax import lax
from jax.experimental import pallas as pl
from jax.experimental.pallas import tpu as pltpu
from jax.sharding import PartitionSpec as P


spacing = 1.0
pbe_kappa = 0.804
pbe_mu = 0.2195149727645171
pbe_beta = 0.06672455060314922
pbe_gamma = 0.031090690869654894
pw_coef = 0.0310907
pw_alpha = 0.2137
pw_first = 7.5957
pw_second = 3.5876
pw_third = 1.6382
pw_fourth = 0.49294

LANES = 128
ROWS = 8


def deriv_matrix(count):
    index = np.arange(count)
    signed = np.where(index < count // 2, index, index - count)
    signed = np.where(index == count // 2, 0, signed)
    waves = signed * (2.0 * math.pi / (count * spacing))
    return np.fft.ifft(1j * waves[:, None] * np.fft.fft(np.eye(count), axis=0), axis=0).real


def split_matrix(count):
    matrix = deriv_matrix(count)
    high = matrix.astype(jnp.bfloat16)
    low = (matrix - high.astype(np.float64)).astype(jnp.bfloat16)
    return jnp.asarray(high), jnp.asarray(low)


def halves(field):
    high = field.astype(jnp.bfloat16)
    return high, (field - high.astype(jnp.float32)).astype(jnp.bfloat16)


def dot(left, right):
    return jnp.dot(left, right, preferred_element_type=jnp.float32)


def matrix_times(high, low, field):
    f_high, f_low = halves(field)
    return dot(high, f_high) + (dot(high, f_low) + dot(low, f_high))


def times_matrix(field, high, low):
    f_high, f_low = halves(field)
    return dot(f_high, high) + (dot(f_low, high) + dot(f_high, low))


def xc_partials(n, g):
    c_fermi = (3.0 * math.pi**2) ** (1.0 / 3.0)
    c_wigner = (3.0 / (4.0 * math.pi)) ** (1.0 / 3.0)
    c_ratio = pbe_beta / pbe_gamma
    v = jnp.exp(jnp.log(n) * (-1.0 / 6.0))
    v2 = v * v
    v4 = v2 * v2
    n13 = n * v4
    v8 = v4 * v4
    v14 = v8 * v4 * v2
    ex = n13 * (-0.75 * c_fermi / math.pi)
    s_scale = (v14 * v2) * (1.0 / (4.0 * c_fermi**2))
    s2 = g * s_scale
    r_x = 1.0 / (pbe_kappa + pbe_mu * s2)
    fx = (1.0 + pbe_kappa) - pbe_kappa**2 * r_x
    dfx = (pbe_mu * pbe_kappa**2) * (r_x * r_x)
    rs = c_wigner * v2
    root = math.sqrt(c_wigner) * v
    q_series = (2.0 * pw_coef) * (
        root * (pw_first + pw_third * rs) + rs * (pw_second + pw_fourth * rs)
    )
    q_slope = (2.0 * pw_coef) * (
        root * (0.5 * pw_first + 1.5 * pw_third * rs) + rs * (pw_second + (2.0 * pw_fourth) * rs)
    )
    r_q = 1.0 / (q_series * (q_series + 1.0))
    log_q = jnp.log(1.0 + (q_series + 1.0) * r_q)
    lead = (2.0 * pw_coef) * (1.0 + pw_alpha * rs)
    ec = -lead * log_q
    nd = (-1.0 / 3.0) * (lead * q_slope * r_q - (2.0 * pw_coef * pw_alpha) * rs * log_q)
    t_scale = v14 * (math.pi / (16.0 * c_fermi))
    t2 = g * t_scale
    grown = jnp.exp(ec * (-1.0 / pbe_gamma))
    r_e = 1.0 / (grown - 1.0)
    factor = c_ratio * r_e
    q = factor * t2
    den = 1.0 + q + q * q
    full = den + c_ratio * t2 * (1.0 + q)
    r_d = 1.0 / (den * full)
    h = pbe_gamma * jnp.log(full * full * r_d)
    h_t = pbe_beta * (1.0 + 2.0 * q) * r_d
    h_p = (-pbe_beta) * (t2 * t2) * (q * (2.0 + q)) * r_d
    energy = n * (ex * fx + ec + h)
    d_grad = n * (ex * dfx * s_scale + h_t * t_scale)
    d_dens = (
        ex * ((4.0 / 3.0) * fx - (8.0 / 3.0) * (s2 * dfx))
        + ec
        + h
        + nd * (1.0 + h_p * factor * grown * r_e * (1.0 / pbe_gamma))
        - (7.0 / 3.0) * t2 * h_t
    )
    return energy, d_dens, d_grad


def slot(axis, step, size, width):
    return pl.multiple_of(lax.rem(lax.axis_index(axis) + step, size) * width, width)


def whole(shape):
    return pl.BlockSpec(shape, lambda s: (0,) * len(shape))


def call(kernel, ins, outs, in_specs=None, scratch=(), flops=1 << 28):
    specs = [whole(a.shape) for a in ins]
    for position, spec in (in_specs or {}).items():
        specs[position] = spec
    return pl.pallas_call(
        kernel,
        grid=(1,),
        in_specs=specs,
        out_specs=[whole(o) for o in outs],
        out_shape=[jax.ShapeDtypeStruct(o, jnp.float32) for o in outs],
        scratch_shapes=list(scratch),
        cost_estimate=pl.CostEstimate(
            flops=flops,
            bytes_accessed=sum(4 * math.prod(o) for o in outs) + sum(4 * a.size for a in ins),
            transcendentals=0,
        ),
    )(*ins)


class Plan:
    def __init__(self, shape):
        self.gx, self.gy = lax.axis_size("gx"), lax.axis_size("gy")
        self.rx, self.ry, self.z = shape
        self.yc = self.ry // self.gx
        self.sx = self.rx // self.gy

    @staticmethod
    def fits(shape, gx, gy):
        rx, ry, z = shape
        return ry % (ROWS * gx) == 0 and ry // gx == ROWS and rx % gy == 0 and (rx // gy) % 2 == 0 and z % (2 * LANES) == 0 and rx % ROWS == 0


def pack_x(plan, density, chunk, lanes):
    def kernel(n_ref, *outs):
        for t, out in enumerate(outs):
            rows = pl.ds(slot("gx", t, plan.gx, plan.yc), plan.yc)
            out[...] = n_ref[:, rows, :].reshape(plan.rx * plan.yc, lanes)

    spec = pl.BlockSpec((plan.rx, plan.ry, lanes), lambda s: (0, 0, chunk))
    return call(kernel, [density], [(plan.rx * plan.yc, lanes)] * plan.gx, {0: spec}, flops=1 << 20)


def pack_y(plan, density):
    def kernel(n_ref, *outs):
        for t, out in enumerate(outs):
            out[...] = n_ref[pl.ds(slot("gy", t, plan.gy, plan.sx), plan.sx)]

    return call(kernel, [density], [(plan.sx, plan.ry, plan.z)] * plan.gy, flops=1 << 20)


def rotate(pieces, axis, size):
    arrived = [pieces[0]] + [None] * (size - 1)
    for t in sorted(range(1, size), key=lambda t: abs(2 * t - size)):
        pairs = [(i, (i + t) % size) for i in range(size)]
        arrived[size - t] = lax.ppermute(pieces[t], axis, pairs)
    return arrived


def after(arrays, token):
    return lax.optimization_barrier((list(arrays), token))[0]


def deriv_x(plan, matrix, pieces, lanes, with_energy):
    gx, rx, yc = plan.gx, plan.rx, plan.yc

    def kernel(high_ref, low_ref, *refs):
        ins, outs = refs[:gx], refs[gx : 2 * gx]
        high, low = high_ref[...], low_ref[...]
        for y in range(0, yc, 2):
            columns = [
                jnp.concatenate([p[pl.ds(y + k, rx, stride=yc), :] for p in ins], axis=0)
                for k in range(2)
            ]
            result = matrix_times(high, low, jnp.concatenate(columns, axis=1))
            for k in range(2):
                for t, out in enumerate(outs):
                    out[pl.ds(y + k, rx, stride=yc), :] = result[
                        t * rx : (t + 1) * rx, k * lanes : (k + 1) * lanes
                    ]
        if with_energy:
            energy_ref, ordered = refs[2 * gx :]
            for t, p in enumerate(ins):
                ordered[pl.ds(slot("gx", t, gx, ROWS), ROWS), :] = p[rx * yc :, :]
            total = ordered[:ROWS, :]
            for t in range(1, gx):
                total = total + ordered[t * ROWS : (t + 1) * ROWS, :]
            energy_ref[...] = total

    outs = [(rx * yc, lanes)] * gx
    scratch = []
    if with_energy:
        outs = outs + [(ROWS, lanes)]
        scratch = [pltpu.VMEM((gx * ROWS, lanes), jnp.float32)]
    return call(kernel, [*matrix, *pieces], outs, scratch=scratch)


def deriv_y(plan, matrix, pieces, lanes, energy=None):
    gy, sx, ry = plan.gy, plan.sx, plan.ry
    together = max(1, 2 * LANES // lanes)
    extra = 0 if energy is None else 1

    def kernel(high_ref, low_ref, *refs):
        ins, outs = refs[extra : extra + gy], refs[extra + gy :]
        high, low = high_ref[...], low_ref[...]
        for x in range(0, sx, together):
            columns = [
                jnp.concatenate([p[x + k] for p in ins], axis=0) for k in range(together)
            ]
            field = columns[0] if together == 1 else jnp.concatenate(columns, axis=1)
            result = matrix_times(high, low, field)
            for k in range(together):
                for t, out in enumerate(outs):
                    out[x + k] = result[t * ry : (t + 1) * ry, k * lanes : (k + 1) * lanes]
        if extra:
            for out in outs:
                out[sx] = jnp.zeros((ry, lanes), jnp.float32)
                out[sx, :ROWS, :] = refs[0][...]

    ins = [*matrix] + ([energy] if extra else []) + list(pieces)
    return call(kernel, ins, [(sx + extra, ry, lanes)] * gy)


def rows_call(kernel, rows, ins, widths, out_width, resident):
    block = rows // 4
    return pl.pallas_call(
        kernel,
        grid=(4,),
        in_specs=[pl.BlockSpec(m.shape, lambda s: (0, 0)) for m in resident]
        + [pl.BlockSpec((block, w), lambda s: (s, 0)) for w in widths],
        out_specs=pl.BlockSpec((block, out_width), lambda s: (s, 0)),
        out_shape=jax.ShapeDtypeStruct((rows, out_width), jnp.float32),
        cost_estimate=pl.CostEstimate(flops=1 << 28, bytes_accessed=1 << 22, transcendentals=0),
    )(*resident, *ins)


def deriv_z(plan, matrix, field):
    def kernel(high_ref, low_ref, f_ref, out_ref):
        out_ref[...] = -times_matrix(f_ref[...], high_ref[...], low_ref[...])

    rows = plan.rx * plan.ry
    flat = field.reshape(rows, plan.z)
    return rows_call(kernel, rows, [flat], [plan.z], plan.z, matrix).reshape(field.shape)


def less_deriv_z(plan, matrix, d_dens, flux):
    def kernel(high_ref, low_ref, *refs):
        count = len(flux)
        dens = jnp.concatenate([r[...] for r in refs[:count]], axis=1)
        field = jnp.concatenate([r[...] for r in refs[count : 2 * count]], axis=1)
        refs[-1][...] = dens + times_matrix(field, high_ref[...], low_ref[...])

    rows = plan.rx * plan.ry
    flat = [a.reshape(rows, a.shape[2]) for a in (*d_dens, *flux)]
    widths = [a.shape[1] for a in flat]
    out = rows_call(kernel, rows, flat, widths, plan.z, matrix)
    return out.reshape(plan.rx, plan.ry, plan.z)


def pointwise(plan, density, grad_z, grad_y, grad_x, chunk, lanes, before):
    gx, gy, rx, ry, yc, sx = plan.gx, plan.gy, plan.rx, plan.ry, plan.yc, plan.sx
    extra = 0 if before is None else 1

    def kernel(*refs):
        n_ref, gz_ref = refs[0], refs[1]
        gy_refs = refs[2 : 2 + gy]
        gx_refs = refs[2 + gy : 2 + gy + gx]
        refs = refs[2 + gy + gx :]
        if extra:
            before_ref, refs = refs[0], refs[1:]
        fx_refs, fy_refs = refs[:gx], refs[gx : gx + gy]
        fz_ref, dd_ref, energy_ref = refs[gx + gy :]
        total = jnp.zeros((yc, lanes), jnp.float32)
        for part in range(gy):
            base = slot("gy", part, gy, sx)

            def step(inner, total, part=part, base=base):
                x = base + inner
                for t in range(gx):
                    rows = pl.ds(slot("gx", t, gx, yc), yc)
                    n = n_ref[x, rows, :]
                    d_x = gx_refs[t][x]
                    d_y = gy_refs[part][inner, rows, :]
                    d_z = gz_ref[x, rows, :]
                    f, d_dens, d_grad = xc_partials(n, d_x * d_x + d_y * d_y + d_z * d_z)
                    twice = 2.0 * d_grad
                    fx_refs[t][x] = twice * d_x
                    fy_refs[part][inner, rows, :] = twice * d_y
                    fz_ref[x, rows, :] = twice * d_z
                    dd_ref[x, rows, :] = d_dens
                    total = total + f
                return total

            total = lax.fori_loop(0, sx, step, total)
        if extra:
            total = total + before_ref[...]
            for out in fx_refs:
                out[rx] = total
        energy_ref[...] = total

    block = pl.BlockSpec((rx, ry, lanes), lambda s: (0, 0, chunk))
    y_block = pl.BlockSpec((sx, ry, lanes), lambda s: (0, 0, chunk))
    specs = {0: block, 1: block} | {2 + t: y_block for t in range(gy)}
    ins = [density, grad_z, *grad_y, *[p.reshape(rx, yc, lanes) for p in grad_x]]
    if extra:
        ins.append(before)
    outs = [(rx + extra, yc, lanes)] * gx + [(sx, ry, lanes)] * gy
    outs += [(rx, ry, lanes)] * 2 + [(yc, lanes)]
    out = call(kernel, ins, outs, specs, flops=1 << 32)
    flux_x = [p.reshape((rx + extra) * yc, lanes) for p in out[:gx]]
    return flux_x, out[gx : gx + gy], out[gx + gy], out[gx + gy + 1], out[gx + gy + 2]


def finish(plan, base, div_x, div_y, lanes, cells):
    gx, gy, rx, ry, yc, sx = plan.gx, plan.gy, plan.rx, plan.ry, plan.yc, plan.sx
    chunks = len(div_x)

    def kernel(base_ref, *refs):
        x_refs = [refs[c * gx : (c + 1) * gx] for c in range(chunks)]
        refs = refs[chunks * gx :]
        y_refs = [refs[c * gy : (c + 1) * gy] for c in range(chunks)]
        out_ref, energy_ref, ordered = refs[chunks * gy :]
        for part in range(gy):
            start = slot("gy", part, gy, sx)

            def step(inner, carry, part=part, start=start):
                x = start + inner
                for c in range(chunks):
                    where = slice(c * lanes, (c + 1) * lanes)
                    for t in range(gx):
                        rows = pl.ds(slot("gx", t, gx, yc), yc)
                        out_ref[x, rows, where] = base_ref[x, rows, where] - (
                            x_refs[c][t][x] + y_refs[c][part][inner, rows, :]
                        )
                return carry

            lax.fori_loop(0, sx, step, 0)
        for t, p in enumerate(y_refs[-1]):
            ordered[pl.ds(slot("gy", t, gy, ROWS), ROWS), :] = p[sx, :ROWS, :]
        total = ordered[:ROWS, :]
        for t in range(1, gy):
            total = total + ordered[t * ROWS : (t + 1) * ROWS, :]
        energy_ref[...] = total

    ins = [base]
    for c in range(chunks):
        ins += [p.reshape(rx, yc, lanes) for p in div_x[c]]
    for c in range(chunks):
        ins += list(div_y[c])
    outs = [(rx, ry, plan.z), (ROWS, lanes)]
    scratch = [pltpu.VMEM((gy * ROWS, lanes), jnp.float32)]
    out, energy = call(kernel, ins, outs, scratch=scratch, flops=1 << 24)
    return out, jnp.sum(energy) / float(cells)


def body(density):
    return tiled_body(density)


def tiled_body(density):
    plan = Plan(density.shape)
    gx, gy = plan.gx, plan.gy
    count_x, count_y, count_z = plan.rx * gx, plan.ry * gy, plan.z
    matrix_x, matrix_y, matrix_z = split_matrix(count_x), split_matrix(count_y), split_matrix(count_z)
    chunks = 2
    lanes = plan.z // chunks

    out = pack_x(plan, density, 0, lanes)
    dens_x = [rotate(out, "gx", gx)]
    out = pack_y(plan, *after([density], out[0]))
    dens_y = rotate(out, "gy", gy)
    for c in range(1, chunks):
        out = pack_x(plan, *after([density], out[0]), c, lanes)
        dens_x.append(rotate(out, "gx", gx))
    grad_z = deriv_z(plan, matrix_z, *after([density], out[0]))
    out = deriv_y(plan, matrix_y, after(dens_y, grad_z), plan.z)
    grad_y = rotate(out, "gy", gy)
    grad_x = []
    for c in range(chunks):
        pieces = after(dens_x[c], out[0])
        out = deriv_x(plan, matrix_x, pieces, lanes, False)
        grad_x.append(rotate(out, "gx", gx))

    token, energy = out[0], None
    flux_x, flux_y, flux_z, d_dens = [], [], [], []
    for c in range(chunks):
        before = energy if c == chunks - 1 else None
        pieces = after(grad_x[c], token)
        f_x, f_y, f_z, dd, energy = pointwise(
            plan, density, grad_z, grad_y, pieces, c, lanes, before
        )
        token = energy
        flux_x.append(rotate(f_x, "gx", gx))
        flux_y.append(rotate(f_y, "gy", gy))
        flux_z.append(f_z)
        d_dens.append(dd)
    base = less_deriv_z(plan, matrix_z, d_dens, flux_z)
    token = base
    div_x, div_y = [], []
    for c in range(chunks):
        last = c == chunks - 1
        out = deriv_x(plan, matrix_x, after(flux_x[c], token), lanes, last)
        div_x.append(rotate(out[:gx], "gx", gx))
        summed = out[gx] if last else None
        out = deriv_y(plan, matrix_y, after(flux_y[c], out[0]), lanes, summed)
        div_y.append(rotate(out, "gy", gy))
        token = out[0]
    return finish(plan, base, div_x, div_y, lanes, count_x * count_y * count_z)


def xc_energy(electrons, grad_sq):
    k_fermi = jnp.cbrt(3.0 * math.pi**2 * electrons)
    exch_unif = -0.75 * k_fermi / math.pi
    s_square = grad_sq / (4.0 * k_fermi**2 * electrons**2)
    enhance = 1.0 + pbe_kappa - pbe_kappa / (1.0 + pbe_mu * s_square / pbe_kappa)
    wigner = jnp.cbrt(3.0 / (4.0 * math.pi * electrons))
    root_rs = jnp.sqrt(wigner)
    series = (
        2.0
        * pw_coef
        * (
            pw_first * root_rs
            + pw_second * wigner
            + pw_third * wigner * root_rs
            + pw_fourth * wigner**2
        )
    )
    corr_unif = -2.0 * pw_coef * (1.0 + pw_alpha * wigner) * jnp.log(1.0 + 1.0 / series)
    screen_sq = 4.0 * k_fermi / math.pi
    t_square = grad_sq / (4.0 * screen_sq * electrons**2)
    factor = pbe_beta / pbe_gamma / jnp.expm1(-corr_unif / pbe_gamma)
    scaled = factor * t_square
    gradient_term = pbe_gamma * jnp.log(
        1.0 + pbe_beta / pbe_gamma * t_square * (1.0 + scaled) / (1.0 + scaled + scaled**2)
    )
    return electrons * (exch_unif * enhance + corr_unif + gradient_term)


def summed_energy(electrons, grad_sq):
    return jnp.sum(xc_energy(electrons, grad_sq))


def total_energy(energy_local, cells):
    return lax.psum(energy_local, ("gx", "gy")) / float(cells)


def wavenum(index, count):
    signed = jnp.where(index < count // 2, index, index - count)
    signed = jnp.where(index == count // 2, 0, signed)
    return signed.astype(jnp.float32) * (2.0 * math.pi / (count * spacing))


def dft_tables(count, order):
    columns = jnp.arange(count, dtype=jnp.int32)
    phase = (order[:, None] * columns[None, :] % count).astype(jnp.float32) * (
        2.0 * math.pi / count
    )
    return (jnp.cos(phase), jnp.sin(phase))


def plain_matrix(count):
    positions = jnp.arange(count, dtype=jnp.int32)
    cosine, sine = dft_tables(count, positions)
    waves = wavenum(positions, count)
    first = jnp.dot(cosine.T * waves[None, :], sine, precision=lax.Precision.HIGHEST)
    second = jnp.dot(sine.T * waves[None, :], cosine, precision=lax.Precision.HIGHEST)
    return (first - second) / float(count)


def plain_body(density):
    count_gx = lax.axis_size("gx")
    count_gy = lax.axis_size("gy")
    rows_x, rows_y, count_z = density.shape
    count_x = rows_x * count_gx
    count_y = rows_y * count_gy
    deriv_x = plain_matrix(count_x)
    deriv_y = plain_matrix(count_y)
    deriv_z = plain_matrix(count_z)

    def line_x(piece):
        flat = piece.reshape(piece.shape[0], piece.shape[1] * piece.shape[2])
        result = jnp.dot(deriv_x, flat, precision=lax.Precision.HIGHEST)
        return result.reshape(piece.shape)

    def line_y(piece):
        turned = jnp.swapaxes(piece, 0, 1)
        flat = turned.reshape(turned.shape[0], turned.shape[1] * turned.shape[2])
        result = jnp.dot(deriv_y, flat, precision=lax.Precision.HIGHEST).reshape(turned.shape)
        return jnp.swapaxes(result, 0, 1)

    def along_x(field):
        lines = line_x(lax.all_to_all(field, "gx", split_axis=2, concat_axis=0, tiled=True))
        return lax.all_to_all(lines, "gx", split_axis=0, concat_axis=2, tiled=True)

    def along_y(field):
        lines = line_y(lax.all_to_all(field, "gy", split_axis=2, concat_axis=1, tiled=True))
        return lax.all_to_all(lines, "gy", split_axis=1, concat_axis=2, tiled=True)

    def along_z(field):
        flat = field.reshape(field.shape[0] * field.shape[1], field.shape[2])
        result = jnp.dot(flat, deriv_z.T, precision=lax.Precision.HIGHEST)
        return result.reshape(field.shape)

    gradients = [along_x(density), along_y(density), along_z(density)]
    grad_sq = (
        gradients[0] * gradients[0] + gradients[1] * gradients[1] + gradients[2] * gradients[2]
    )
    energy_local, partials = jax.value_and_grad(summed_energy, argnums=(0, 1))(density, grad_sq)
    d_dens, d_grad = partials
    fluxes = [2.0 * d_grad * gradient for gradient in gradients]
    divergence = along_x(fluxes[0]) + along_y(fluxes[1]) + along_z(fluxes[2])
    potential = d_dens - divergence
    return (potential, total_energy(energy_local, count_x * count_y * count_z))


def solution(mesh):
    in_specs = (P("gx", "gy", None),)
    out_specs = (P("gx", "gy", None), P())

    def run(density):
        gx, gy = mesh.shape["gx"], mesh.shape["gy"]
        x, y, z = density.shape
        tiled = Plan.fits((x // gx, y // gy, z), gx, gy)
        step = jax.shard_map(
            body if tiled else plain_body,
            mesh=mesh,
            in_specs=in_specs,
            out_specs=out_specs,
            check_vma=False,
        )
        return step(density)

    return run
```

```python
import math

import jax
import jax.numpy as jnp
import numpy as np
from jax import lax
from jax.experimental import pallas as pl
from jax.experimental.pallas import tpu as pltpu
from jax.sharding import PartitionSpec as P


spacing = 1.0
pbe_kappa = 0.804
pbe_mu = 0.2195149727645171
pbe_beta = 0.06672455060314922
pbe_gamma = 0.031090690869654894
pw_coef = 0.0310907
pw_alpha = 0.2137
pw_first = 7.5957
pw_second = 3.5876
pw_third = 1.6382
pw_fourth = 0.49294

LANES = 128
ROWS = 8


def deriv_matrix(count):
    index = np.arange(count)
    signed = np.where(index < count // 2, index, index - count)
    signed = np.where(index == count // 2, 0, signed)
    waves = signed * (2.0 * math.pi / (count * spacing))
    return np.fft.ifft(1j * waves[:, None] * np.fft.fft(np.eye(count), axis=0), axis=0).real


def split_matrix(count):
    matrix = deriv_matrix(count)
    high = matrix.astype(jnp.bfloat16)
    low = (matrix - high.astype(np.float64)).astype(jnp.bfloat16)
    return jnp.asarray(high), jnp.asarray(low)


def halves(field):
    high = field.astype(jnp.bfloat16)
    return high, (field - high.astype(jnp.float32)).astype(jnp.bfloat16)


def dot(left, right):
    return jnp.dot(left, right, preferred_element_type=jnp.float32)


def matrix_times(high, low, field):
    f_high, f_low = halves(field)
    return dot(high, f_high) + (dot(high, f_low) + dot(low, f_high))


def times_matrix(field, high, low):
    f_high, f_low = halves(field)
    return dot(f_high, high) + (dot(f_low, high) + dot(f_high, low))


def xc_partials(n, g):
    c_fermi = (3.0 * math.pi**2) ** (1.0 / 3.0)
    c_wigner = (3.0 / (4.0 * math.pi)) ** (1.0 / 3.0)
    c_ratio = pbe_beta / pbe_gamma
    v = jnp.exp(jnp.log(n) * (-1.0 / 6.0))
    v2 = v * v
    v4 = v2 * v2
    n13 = n * v4
    v8 = v4 * v4
    v14 = v8 * v4 * v2
    ex = n13 * (-0.75 * c_fermi / math.pi)
    s_scale = (v14 * v2) * (1.0 / (4.0 * c_fermi**2))
    s2 = g * s_scale
    r_x = 1.0 / (pbe_kappa + pbe_mu * s2)
    fx = (1.0 + pbe_kappa) - pbe_kappa**2 * r_x
    dfx = (pbe_mu * pbe_kappa**2) * (r_x * r_x)
    rs = c_wigner * v2
    root = math.sqrt(c_wigner) * v
    q_series = (2.0 * pw_coef) * (
        root * (pw_first + pw_third * rs) + rs * (pw_second + pw_fourth * rs)
    )
    q_slope = (2.0 * pw_coef) * (
        root * (0.5 * pw_first + 1.5 * pw_third * rs) + rs * (pw_second + (2.0 * pw_fourth) * rs)
    )
    r_q = 1.0 / (q_series * (q_series + 1.0))
    log_q = jnp.log(1.0 + (q_series + 1.0) * r_q)
    lead = (2.0 * pw_coef) * (1.0 + pw_alpha * rs)
    ec = -lead * log_q
    nd = (-1.0 / 3.0) * (lead * q_slope * r_q - (2.0 * pw_coef * pw_alpha) * rs * log_q)
    t_scale = v14 * (math.pi / (16.0 * c_fermi))
    t2 = g * t_scale
    grown = jnp.exp(ec * (-1.0 / pbe_gamma))
    r_e = 1.0 / (grown - 1.0)
    factor = c_ratio * r_e
    q = factor * t2
    den = 1.0 + q + q * q
    full = den + c_ratio * t2 * (1.0 + q)
    r_d = 1.0 / (den * full)
    h = pbe_gamma * jnp.log(full * full * r_d)
    h_t = pbe_beta * (1.0 + 2.0 * q) * r_d
    h_p = (-pbe_beta) * (t2 * t2) * (q * (2.0 + q)) * r_d
    energy = n * (ex * fx + ec + h)
    d_grad = n * (ex * dfx * s_scale + h_t * t_scale)
    d_dens = (
        ex * ((4.0 / 3.0) * fx - (8.0 / 3.0) * (s2 * dfx))
        + ec
        + h
        + nd * (1.0 + h_p * factor * grown * r_e * (1.0 / pbe_gamma))
        - (7.0 / 3.0) * t2 * h_t
    )
    return energy, d_dens, d_grad


def slot(axis, step, size, width):
    return pl.multiple_of(lax.rem(lax.axis_index(axis) + step, size) * width, width)


def whole(shape):
    return pl.BlockSpec(shape, lambda s: (0,) * len(shape))


def call(kernel, ins, outs, in_specs=None, scratch=(), flops=1 << 28):
    specs = [whole(a.shape) for a in ins]
    for position, spec in (in_specs or {}).items():
        specs[position] = spec
    return pl.pallas_call(
        kernel,
        grid=(1,),
        in_specs=specs,
        out_specs=[whole(o) for o in outs],
        out_shape=[jax.ShapeDtypeStruct(o, jnp.float32) for o in outs],
        scratch_shapes=list(scratch),
        cost_estimate=pl.CostEstimate(
            flops=flops,
            bytes_accessed=sum(4 * math.prod(o) for o in outs) + sum(4 * a.size for a in ins),
            transcendentals=0,
        ),
    )(*ins)


class Plan:
    def __init__(self, shape):
        self.gx, self.gy = lax.axis_size("gx"), lax.axis_size("gy")
        self.rx, self.ry, self.z = shape
        self.yc = self.ry // self.gx
        self.sx = self.rx // self.gy

    @staticmethod
    def fits(shape, gx, gy):
        rx, ry, z = shape
        return ry % (ROWS * gx) == 0 and ry // gx == ROWS and rx % gy == 0 and (rx // gy) % 2 == 0 and z % (2 * LANES) == 0 and rx % ROWS == 0


class Blocks:
    def __init__(self, plan, stacked):
        self.plan, self.stacked = plan, stacked
        self.count = 1 if stacked else plan.gx

    def shapes(self, *piece):
        return [(self.plan.gx, *piece)] if self.stacked else [piece] * self.plan.gx

    def views(self, refs):
        return [refs[0].at[d] for d in range(self.plan.gx)] if self.stacked else list(refs)

    def rows(self, t):
        yc = self.plan.yc
        return pl.ds(t * yc if self.stacked else slot("gx", t, self.plan.gx, yc), yc)

    def shaped(self, arrays, *piece):
        lead = (self.plan.gx,) if self.stacked else ()
        return [a.reshape(*lead, *piece) for a in arrays]


def pack_x(plan, density, chunk, lanes, stacked):
    blocks = Blocks(plan, stacked)

    def kernel(n_ref, *outs):
        for t, out in enumerate(blocks.views(outs)):
            out[...] = n_ref[:, blocks.rows(t), :].reshape(plan.rx * plan.yc, lanes)

    spec = pl.BlockSpec((plan.rx, plan.ry, lanes), lambda s: (0, 0, chunk))
    outs = blocks.shapes(plan.rx * plan.yc, lanes)
    return call(kernel, [density], outs, {0: spec}, flops=1 << 20)


def pack_y(plan, density):
    def kernel(n_ref, *outs):
        for t, out in enumerate(outs):
            out[...] = n_ref[pl.ds(slot("gy", t, plan.gy, plan.sx), plan.sx)]

    return call(kernel, [density], [(plan.sx, plan.ry, plan.z)] * plan.gy, flops=1 << 20)


def rotate(pieces, axis, size):
    arrived = [pieces[0]] + [None] * (size - 1)
    for t in sorted(range(1, size), key=lambda t: abs(2 * t - size)):
        pairs = [(i, (i + t) % size) for i in range(size)]
        arrived[size - t] = lax.ppermute(pieces[t], axis, pairs)
    return arrived


def exchange(pieces, axis):
    return [lax.all_to_all(pieces[0], axis, 0, 0, tiled=True)]


def after(arrays, token):
    return lax.optimization_barrier((list(arrays), token))[0]


def ordered_sum(pieces, axis, size, scratch):
    for t, piece in enumerate(pieces):
        scratch[pl.ds(slot(axis, t, size, ROWS), ROWS), :] = piece
    total = scratch[:ROWS, :]
    for t in range(1, size):
        total = total + scratch[t * ROWS : (t + 1) * ROWS, :]
    return total


def deriv_x(plan, matrix, pieces, lanes, stacked, energy=None):
    rx, yc = plan.rx, plan.yc
    extra = 0 if energy is None else 1
    blocks = Blocks(plan, stacked)

    def kernel(high_ref, low_ref, *refs):
        ins = blocks.views(refs[extra : extra + blocks.count])
        outs = blocks.views(refs[extra + blocks.count :])
        high, low = high_ref[...], low_ref[...]
        for y in range(0, yc, 2):
            columns = [
                jnp.concatenate([p[pl.ds(y + k, rx, stride=yc), :] for p in ins], axis=0)
                for k in range(2)
            ]
            result = matrix_times(high, low, jnp.concatenate(columns, axis=1))
            for k in range(2):
                for t, out in enumerate(outs):
                    out[pl.ds(y + k, rx, stride=yc), :] = result[
                        t * rx : (t + 1) * rx, k * lanes : (k + 1) * lanes
                    ]
        if extra:
            for out in outs:
                out[rx * yc :, :] = refs[0][...]

    outs = blocks.shapes((rx + extra) * yc, lanes)
    ins = [*matrix] + ([energy] if extra else []) + list(pieces)
    return call(kernel, ins, outs)


def deriv_y(plan, matrix, pieces, lanes, with_energy=False):
    gy, sx, ry = plan.gy, plan.sx, plan.ry
    together = max(1, 2 * LANES // lanes)

    def kernel(high_ref, low_ref, *refs):
        ins, outs = refs[:gy], refs[gy : 2 * gy]
        high, low = high_ref[...], low_ref[...]
        for x in range(0, sx, together):
            columns = [
                jnp.concatenate([p[x + k] for p in ins], axis=0) for k in range(together)
            ]
            field = columns[0] if together == 1 else jnp.concatenate(columns, axis=1)
            result = matrix_times(high, low, field)
            for k in range(together):
                for t, out in enumerate(outs):
                    out[x + k] = result[t * ry : (t + 1) * ry, k * lanes : (k + 1) * lanes]
        if with_energy:
            energy_ref, ordered = refs[2 * gy :]
            energy_ref[...] = ordered_sum([p[sx, :ROWS, :] for p in ins], "gy", gy, ordered)

    outs, scratch = [(sx, ry, lanes)] * gy, []
    if with_energy:
        outs = outs + [(ROWS, lanes)]
        scratch = [pltpu.VMEM((gy * ROWS, lanes), jnp.float32)]
    return call(kernel, [*matrix, *pieces], outs, scratch=scratch)


def rows_call(kernel, rows, ins, widths, out_width, resident):
    block = rows // 4
    return pl.pallas_call(
        kernel,
        grid=(4,),
        in_specs=[pl.BlockSpec(m.shape, lambda s: (0, 0)) for m in resident]
        + [pl.BlockSpec((block, w), lambda s: (s, 0)) for w in widths],
        out_specs=pl.BlockSpec((block, out_width), lambda s: (s, 0)),
        out_shape=jax.ShapeDtypeStruct((rows, out_width), jnp.float32),
        cost_estimate=pl.CostEstimate(flops=1 << 28, bytes_accessed=1 << 22, transcendentals=0),
    )(*resident, *ins)


def deriv_z(plan, matrix, field):
    def kernel(high_ref, low_ref, f_ref, out_ref):
        out_ref[...] = -times_matrix(f_ref[...], high_ref[...], low_ref[...])

    rows = plan.rx * plan.ry
    flat = field.reshape(rows, plan.z)
    return rows_call(kernel, rows, [flat], [plan.z], plan.z, matrix).reshape(field.shape)


def add_flux_z(plan, matrix, flux, chunk, lanes, terms):
    rows = plan.rx * plan.ry
    flat = [a.reshape(rows, -1) for a in (flux, *terms)]

    def kernel(high_ref, low_ref, f_ref, *refs):
        own = slice(chunk * lanes, (chunk + 1) * lanes)
        total = times_matrix(f_ref[...], high_ref[own, :], low_ref[own, :])
        if len(refs) > 1:
            total = total + refs[0][...] + jnp.concatenate([r[...] for r in refs[1:-1]], axis=1)
        refs[-1][...] = total

    widths = [a.shape[1] for a in flat]
    out = rows_call(kernel, rows, flat, widths, plan.z, matrix)
    return out.reshape(plan.rx, plan.ry, plan.z)


def pointwise(plan, density, grad_z, grad_y, grad_x, chunk, lanes, stacked, before):
    gx, gy, rx, ry, yc, sx = plan.gx, plan.gy, plan.rx, plan.ry, plan.yc, plan.sx
    extra = 0 if before is None else 1
    blocks = Blocks(plan, stacked)

    def kernel(*refs):
        n_ref, gz_ref = refs[0], refs[1]
        gy_refs = refs[2 : 2 + gy]
        gx_refs = blocks.views(refs[2 + gy : 2 + gy + blocks.count])
        refs = refs[2 + gy + blocks.count :]
        if extra:
            before_ref, refs = refs[0], refs[1:]
        fx_refs, refs = blocks.views(refs[: blocks.count]), refs[blocks.count :]
        fy_refs = refs[:gy]
        fz_ref, dd_ref, energy_ref = refs[gy:]
        total = jnp.zeros((yc, lanes), jnp.float32)
        for part in range(gy):
            base = slot("gy", part, gy, sx)

            def step(inner, total, part=part, base=base):
                x = base + inner
                for t in range(gx):
                    rows = blocks.rows(t)
                    n = n_ref[x, rows, :]
                    d_x = gx_refs[t][x]
                    d_y = gy_refs[part][inner, rows, :]
                    d_z = gz_ref[x, rows, :]
                    f, d_dens, d_grad = xc_partials(n, d_x * d_x + d_y * d_y + d_z * d_z)
                    twice = 2.0 * d_grad
                    fx_refs[t][x] = twice * d_x
                    fy_refs[part][inner, rows, :] = twice * d_y
                    fz_ref[x, rows, :] = twice * d_z
                    dd_ref[x, rows, :] = d_dens
                    total = total + f
                return total

            total = lax.fori_loop(0, sx, step, total)
        if extra:
            total = total + before_ref[...]
            for out in fy_refs:
                out[sx] = jnp.zeros((ry, lanes), jnp.float32)
                out[sx, :ROWS, :] = total
        energy_ref[...] = total

    block = pl.BlockSpec((rx, ry, lanes), lambda s: (0, 0, chunk))
    y_block = pl.BlockSpec((sx, ry, lanes), lambda s: (0, 0, chunk))
    specs = {0: block, 1: block} | {2 + t: y_block for t in range(gy)}
    ins = [density, grad_z, *grad_y, *blocks.shaped(grad_x, rx, yc, lanes)]
    if extra:
        ins.append(before)
    outs = blocks.shapes(rx, yc, lanes) + [(sx + extra, ry, lanes)] * gy
    outs += [(rx, ry, lanes)] * 2 + [(yc, lanes)]
    out = call(kernel, ins, outs, specs, flops=1 << 32)
    flux_x = blocks.shaped(out[: blocks.count], rx * yc, lanes)
    return flux_x, out[blocks.count : blocks.count + gy], *out[blocks.count + gy :]


def less_y(plan, base, div_y, lanes):
    gy, rx, ry, sx = plan.gy, plan.rx, plan.ry, plan.sx

    def kernel(base_ref, *refs):
        out_ref = refs[-1]
        for part in range(gy):
            rows = pl.ds(slot("gy", part, gy, sx), sx)
            for c in range(len(div_y)):
                where = slice(c * lanes, (c + 1) * lanes)
                out_ref[rows, :, where] = base_ref[rows, :, where] - refs[c * gy + part][...]

    ins = [base] + [p for pieces in div_y for p in pieces]
    return call(kernel, ins, [(rx, ry, plan.z)], flops=1 << 24)[0]


def finish(plan, base, div_x, chunk, lanes, stacked, before, scale):
    gx, rx, ry, yc = plan.gx, plan.rx, plan.ry, plan.yc
    last = scale is not None
    blocks = Blocks(plan, stacked)

    def kernel(base_ref, *refs):
        x_refs, refs = blocks.views(refs[: blocks.count]), refs[blocks.count :]
        out_ref = refs[1] if last else refs[0]
        for t in range(gx):
            rows = blocks.rows(t)
            out_ref[:, rows, :] = base_ref[:, rows, :] - x_refs[t][:rx]
        if last:
            energy_ref, ordered = refs[2:]
            total = ordered_sum([p[rx] for p in x_refs], "gx", gx, ordered)
            energy_ref[0, 0] = jnp.sum(total) * scale

    block = pl.BlockSpec((rx, ry, lanes), lambda s: (0, 0, chunk))
    ins = [base, *blocks.shaped(div_x, rx + (1 if last else 0), yc, lanes)]
    specs = [block] + [whole(a.shape) for a in ins[1:]]
    out_shape = [jax.ShapeDtypeStruct((rx, ry, plan.z), jnp.float32)]
    out_specs, scratch, aliases = [block], [], {}
    if last:
        aliases = {len(ins): 0}
        ins.append(before)
        specs.append(pl.BlockSpec(memory_space=pl.ANY))
        out_shape.append(jax.ShapeDtypeStruct((1, 1), jnp.float32))
        out_specs.append(pl.BlockSpec(memory_space=pltpu.SMEM))
        scratch = [pltpu.VMEM((gx * ROWS, lanes), jnp.float32)]
    return pl.pallas_call(
        kernel,
        grid=(1,),
        in_specs=specs,
        out_specs=out_specs,
        out_shape=out_shape,
        scratch_shapes=scratch,
        input_output_aliases=aliases,
        cost_estimate=pl.CostEstimate(flops=1 << 24, bytes_accessed=1 << 22, transcendentals=0),
        name="finish",
    )(*ins)


def body(density):
    return tiled_body(density)


def tiled_body(density):
    plan = Plan(density.shape)
    gx, gy = plan.gx, plan.gy
    count_x, count_y, count_z = plan.rx * gx, plan.ry * gy, plan.z
    matrix_x, matrix_y, matrix_z = split_matrix(count_x), split_matrix(count_y), split_matrix(count_z)
    lanes = plan.z // 2

    out = pack_x(plan, density, 0, lanes, True)
    dens_0 = exchange(out, "gx")
    out = pack_y(plan, *after([density], out[0]))
    dens_y = rotate(out, "gy", gy)
    packed = pack_x(plan, *after([density], out[0]), 1, lanes, False)
    grad_z = deriv_z(plan, matrix_z, *after([density], packed[0]))
    dens_1 = rotate(after(packed, grad_z), "gx", gx)
    out_x = deriv_x(plan, matrix_x, after(dens_0, grad_z), lanes, True)
    grad_0 = exchange(out_x, "gx")
    out = deriv_y(plan, matrix_y, after(dens_y, out_x[0]), plan.z)
    grad_y = rotate(out, "gy", gy)
    out_x = deriv_x(plan, matrix_x, after(dens_1, out[0]), lanes, False)
    grad_1 = rotate(out_x, "gx", gx)
    grad_0 = after(grad_0, out_x[0])
    f_x, f_y, f_z, part_0, energy = pointwise(
        plan, density, grad_z, grad_y, grad_0, 0, lanes, True, None
    )
    flux_0 = exchange(f_x, "gx")
    flux_y = [rotate(f_y, "gy", gy)]
    base = add_flux_z(plan, matrix_z, *after([f_z], energy), 0, lanes, [])
    grad_1 = after(grad_1, base)
    f_x, f_y, f_z, part_1, energy = pointwise(
        plan, density, grad_z, grad_y, grad_1, 1, lanes, False, energy
    )
    flux_1 = rotate(f_x, "gx", gx)
    flux_y.append(rotate(f_y, "gy", gy))
    terms = [base, part_0, part_1]
    base = add_flux_z(plan, matrix_z, *after([f_z], energy), 1, lanes, terms)
    out_x = deriv_x(plan, matrix_x, after(flux_0, base), lanes, True)
    div_0 = exchange(out_x, "gx")
    out = deriv_y(plan, matrix_y, after(flux_y[0], out_x[0]), lanes)
    div_y = [rotate(out, "gy", gy)]
    *out, energy = deriv_y(plan, matrix_y, after(flux_y[1], out[0]), lanes, True)
    div_y.append(rotate(out, "gy", gy))
    out_x = deriv_x(plan, matrix_x, after(flux_1, out[0]), lanes, False, energy)
    div_1 = rotate(out_x, "gx", gx)
    base = less_y(plan, *after([base], out_x[0]), div_y, lanes)
    scale = 1.0 / float(count_x * count_y * count_z)
    (half,) = finish(plan, base, div_0, 0, lanes, True, None, None)
    done, energy = finish(plan, base, div_1, 1, lanes, False, half, scale)
    return done, energy[0, 0]


def xc_energy(electrons, grad_sq):
    k_fermi = jnp.cbrt(3.0 * math.pi**2 * electrons)
    exch_unif = -0.75 * k_fermi / math.pi
    s_square = grad_sq / (4.0 * k_fermi**2 * electrons**2)
    enhance = 1.0 + pbe_kappa - pbe_kappa / (1.0 + pbe_mu * s_square / pbe_kappa)
    wigner = jnp.cbrt(3.0 / (4.0 * math.pi * electrons))
    root_rs = jnp.sqrt(wigner)
    series = (
        2.0
        * pw_coef
        * (
            pw_first * root_rs
            + pw_second * wigner
            + pw_third * wigner * root_rs
            + pw_fourth * wigner**2
        )
    )
    corr_unif = -2.0 * pw_coef * (1.0 + pw_alpha * wigner) * jnp.log(1.0 + 1.0 / series)
    screen_sq = 4.0 * k_fermi / math.pi
    t_square = grad_sq / (4.0 * screen_sq * electrons**2)
    factor = pbe_beta / pbe_gamma / jnp.expm1(-corr_unif / pbe_gamma)
    scaled = factor * t_square
    gradient_term = pbe_gamma * jnp.log(
        1.0 + pbe_beta / pbe_gamma * t_square * (1.0 + scaled) / (1.0 + scaled + scaled**2)
    )
    return electrons * (exch_unif * enhance + corr_unif + gradient_term)


def summed_energy(electrons, grad_sq):
    return jnp.sum(xc_energy(electrons, grad_sq))


def total_energy(energy_local, cells):
    return lax.psum(energy_local, ("gx", "gy")) / float(cells)


def wavenum(index, count):
    signed = jnp.where(index < count // 2, index, index - count)
    signed = jnp.where(index == count // 2, 0, signed)
    return signed.astype(jnp.float32) * (2.0 * math.pi / (count * spacing))


def dft_tables(count, order):
    columns = jnp.arange(count, dtype=jnp.int32)
    phase = (order[:, None] * columns[None, :] % count).astype(jnp.float32) * (
        2.0 * math.pi / count
    )
    return (jnp.cos(phase), jnp.sin(phase))


def plain_matrix(count):
    positions = jnp.arange(count, dtype=jnp.int32)
    cosine, sine = dft_tables(count, positions)
    waves = wavenum(positions, count)
    first = jnp.dot(cosine.T * waves[None, :], sine, precision=lax.Precision.HIGHEST)
    second = jnp.dot(sine.T * waves[None, :], cosine, precision=lax.Precision.HIGHEST)
    return (first - second) / float(count)


def plain_body(density):
    count_gx = lax.axis_size("gx")
    count_gy = lax.axis_size("gy")
    rows_x, rows_y, count_z = density.shape
    count_x = rows_x * count_gx
    count_y = rows_y * count_gy
    deriv_x = plain_matrix(count_x)
    deriv_y = plain_matrix(count_y)
    deriv_z = plain_matrix(count_z)

    def line_x(piece):
        flat = piece.reshape(piece.shape[0], piece.shape[1] * piece.shape[2])
        result = jnp.dot(deriv_x, flat, precision=lax.Precision.HIGHEST)
        return result.reshape(piece.shape)

    def line_y(piece):
        turned = jnp.swapaxes(piece, 0, 1)
        flat = turned.reshape(turned.shape[0], turned.shape[1] * turned.shape[2])
        result = jnp.dot(deriv_y, flat, precision=lax.Precision.HIGHEST).reshape(turned.shape)
        return jnp.swapaxes(result, 0, 1)

    def along_x(field):
        lines = line_x(lax.all_to_all(field, "gx", split_axis=2, concat_axis=0, tiled=True))
        return lax.all_to_all(lines, "gx", split_axis=0, concat_axis=2, tiled=True)

    def along_y(field):
        lines = line_y(lax.all_to_all(field, "gy", split_axis=2, concat_axis=1, tiled=True))
        return lax.all_to_all(lines, "gy", split_axis=1, concat_axis=2, tiled=True)

    def along_z(field):
        flat = field.reshape(field.shape[0] * field.shape[1], field.shape[2])
        result = jnp.dot(flat, deriv_z.T, precision=lax.Precision.HIGHEST)
        return result.reshape(field.shape)

    gradients = [along_x(density), along_y(density), along_z(density)]
    grad_sq = (
        gradients[0] * gradients[0] + gradients[1] * gradients[1] + gradients[2] * gradients[2]
    )
    energy_local, partials = jax.value_and_grad(summed_energy, argnums=(0, 1))(density, grad_sq)
    d_dens, d_grad = partials
    fluxes = [2.0 * d_grad * gradient for gradient in gradients]
    divergence = along_x(fluxes[0]) + along_y(fluxes[1]) + along_z(fluxes[2])
    potential = d_dens - divergence
    return (potential, total_energy(energy_local, count_x * count_y * count_z))


def solution(mesh):
    in_specs = (P("gx", "gy", None),)
    out_specs = (P("gx", "gy", None), P())

    def run(density):
        gx, gy = mesh.shape["gx"], mesh.shape["gy"]
        x, y, z = density.shape
        tiled = Plan.fits((x // gx, y // gy, z), gx, gy)
        step = jax.shard_map(
            body if tiled else plain_body,
            mesh=mesh,
            in_specs=in_specs,
            out_specs=out_specs,
            check_vma=False,
        )
        return step(density)

    return run
```

```python
import math

import jax
import jax.numpy as jnp
import numpy as np
from jax import lax
from jax.experimental import pallas as pl
from jax.experimental.pallas import tpu as pltpu
from jax.sharding import PartitionSpec as P


spacing = 1.0
pbe_kappa = 0.804
pbe_mu = 0.2195149727645171
pbe_beta = 0.06672455060314922
pbe_gamma = 0.031090690869654894
pw_coef = 0.0310907
pw_alpha = 0.2137
pw_first = 7.5957
pw_second = 3.5876
pw_third = 1.6382
pw_fourth = 0.49294

GRANT = 16 << 20
LANES = 128
ROWS = 8


def deriv_matrix(count):
    index = np.arange(count)
    signed = np.where(index < count // 2, index, index - count)
    signed = np.where(index == count // 2, 0, signed)
    waves = signed * (2.0 * math.pi / (count * spacing))
    return np.fft.ifft(1j * waves[:, None] * np.fft.fft(np.eye(count), axis=0), axis=0).real


def split_matrix(count):
    matrix = deriv_matrix(count)
    high = matrix.astype(jnp.bfloat16)
    low = (matrix - high.astype(np.float64)).astype(jnp.bfloat16)
    return jnp.asarray(high), jnp.asarray(low)


def halves(field):
    high = field.astype(jnp.bfloat16)
    return high, (field - high.astype(jnp.float32)).astype(jnp.bfloat16)


def dot(left, right):
    return jnp.dot(left, right, preferred_element_type=jnp.float32)


def matrix_times(high, low, field):
    f_high, f_low = halves(field)
    return dot(high, f_high) + (dot(high, f_low) + dot(low, f_high))


def times_matrix(field, high, low):
    f_high, f_low = halves(field)
    return dot(f_high, high) + (dot(f_low, high) + dot(f_high, low))


def xc_partials(n, g):
    c_fermi = (3.0 * math.pi**2) ** (1.0 / 3.0)
    c_wigner = (3.0 / (4.0 * math.pi)) ** (1.0 / 3.0)
    c_ratio = pbe_beta / pbe_gamma
    v = jnp.exp(jnp.log(n) * (-1.0 / 6.0))
    v2 = v * v
    v4 = v2 * v2
    n13 = n * v4
    v8 = v4 * v4
    v14 = v8 * v4 * v2
    ex = n13 * (-0.75 * c_fermi / math.pi)
    s_scale = (v14 * v2) * (1.0 / (4.0 * c_fermi**2))
    s2 = g * s_scale
    r_x = 1.0 / (pbe_kappa + pbe_mu * s2)
    fx = (1.0 + pbe_kappa) - pbe_kappa**2 * r_x
    dfx = (pbe_mu * pbe_kappa**2) * (r_x * r_x)
    rs = c_wigner * v2
    root = math.sqrt(c_wigner) * v
    q_series = (2.0 * pw_coef) * (
        root * (pw_first + pw_third * rs) + rs * (pw_second + pw_fourth * rs)
    )
    q_slope = (2.0 * pw_coef) * (
        root * (0.5 * pw_first + 1.5 * pw_third * rs) + rs * (pw_second + (2.0 * pw_fourth) * rs)
    )
    r_q = 1.0 / (q_series * (q_series + 1.0))
    log_q = jnp.log(1.0 + (q_series + 1.0) * r_q)
    lead = (2.0 * pw_coef) * (1.0 + pw_alpha * rs)
    ec = -lead * log_q
    nd = (-1.0 / 3.0) * (lead * q_slope * r_q - (2.0 * pw_coef * pw_alpha) * rs * log_q)
    t_scale = v14 * (math.pi / (16.0 * c_fermi))
    t2 = g * t_scale
    grown = jnp.exp(ec * (-1.0 / pbe_gamma))
    r_e = 1.0 / (grown - 1.0)
    factor = c_ratio * r_e
    q = factor * t2
    den = 1.0 + q + q * q
    full = den + c_ratio * t2 * (1.0 + q)
    r_d = 1.0 / (den * full)
    h = pbe_gamma * jnp.log(full * full * r_d)
    h_t = pbe_beta * (1.0 + 2.0 * q) * r_d
    h_p = (-pbe_beta) * (t2 * t2) * (q * (2.0 + q)) * r_d
    energy = n * (ex * fx + ec + h)
    d_grad = n * (ex * dfx * s_scale + h_t * t_scale)
    d_dens = (
        ex * ((4.0 / 3.0) * fx - (8.0 / 3.0) * (s2 * dfx))
        + ec
        + h
        + nd * (1.0 + h_p * factor * grown * r_e * (1.0 / pbe_gamma))
        - (7.0 / 3.0) * t2 * h_t
    )
    return energy, d_dens, d_grad


def slot(axis, step, size, width):
    return pl.multiple_of(lax.rem(lax.axis_index(axis) + step, size) * width, width)


VMEM = pl.BlockSpec(memory_space=pltpu.VMEM)
HBM = pl.BlockSpec(memory_space=pltpu.HBM)


def call(kernel, ins, outs, scratch=(), flops=1 << 28):
    return pl.pallas_call(
        kernel,
        in_specs=[VMEM] * len(ins),
        out_specs=[VMEM] * len(outs),
        out_shape=[jax.ShapeDtypeStruct(o, jnp.float32) for o in outs],
        scratch_shapes=list(scratch),
        cost_estimate=pl.CostEstimate(
            flops=flops,
            bytes_accessed=sum(4 * math.prod(o) for o in outs) + sum(4 * a.size for a in ins),
            transcendentals=0,
        ),
        compiler_params=pltpu.CompilerParams(vmem_limit_bytes=GRANT),
    )(*ins)


def pack(field, outs, parts, grant=GRANT):
    def kernel(field_ref, *refs):
        out_refs, semaphore = refs[:-1], refs[-1]
        copies = [
            pltpu.make_async_copy(field_ref.at[part], out, semaphore.at[k])
            for k, (part, out) in enumerate(zip(parts(), out_refs))
        ]
        for copy in copies:
            copy.start()
        for copy in copies:
            copy.wait()

    return pl.pallas_call(
        kernel,
        in_specs=[pl.BlockSpec(memory_space=pl.ANY)],
        out_specs=[VMEM] * len(outs),
        out_shape=[jax.ShapeDtypeStruct(o, jnp.float32) for o in outs],
        scratch_shapes=[pltpu.SemaphoreType.DMA((len(outs),))],
        cost_estimate=pl.CostEstimate(flops=1 << 20, bytes_accessed=1 << 22, transcendentals=0),
        compiler_params=pltpu.CompilerParams(vmem_limit_bytes=grant),
    )(field)


class Plan:
    def __init__(self, shape):
        self.gx, self.gy = lax.axis_size("gx"), lax.axis_size("gy")
        self.rx, self.ry, self.z = shape
        self.yc = self.ry // self.gx
        self.sx = self.rx // self.gy

    @staticmethod
    def fits(shape, gx, gy):
        rx, ry, z = shape
        return ry % (ROWS * gx) == 0 and ry // gx == ROWS and rx % gy == 0 and (rx // gy) % 2 == 0 and z % (2 * LANES) == 0 and rx % ROWS == 0


def chunk_rows(plan, t):
    return pl.ds(slot("gx", t, plan.gx, plan.yc), plan.yc)


def pack_x(plan, density, chunk, lanes):
    def parts():
        own = pl.ds(chunk * lanes, lanes)
        return [(slice(None), chunk_rows(plan, t), own) for t in range(plan.gx)]

    outs = [(plan.rx, plan.yc, lanes)] * plan.gx
    grant = None if chunk == 0 else GRANT
    out = pack(density, outs, parts, grant)
    return [p.reshape(plan.rx * plan.yc, lanes) for p in out]


def pack_y(plan, density):
    def parts():
        return [(pl.ds(slot("gy", t, plan.gy, plan.sx), plan.sx),) for t in range(plan.gy)]

    return pack(density, [(plan.sx, plan.ry, plan.z)] * plan.gy, parts)


def rotate(pieces, axis, size):
    arrived = [pieces[0]] + [None] * (size - 1)
    for t in sorted(range(1, size), key=lambda t: abs(2 * t - size)):
        pairs = [(i, (i + t) % size) for i in range(size)]
        arrived[size - t] = lax.ppermute(pieces[t], axis, pairs)
    return arrived


def after(arrays, token):
    return lax.optimization_barrier((list(arrays), token))[0]


def ordered_sum(pieces, axis, size, scratch):
    for t, piece in enumerate(pieces):
        scratch[pl.ds(slot(axis, t, size, ROWS), ROWS), :] = piece
    total = scratch[:ROWS, :]
    for t in range(1, size):
        total = total + scratch[t * ROWS : (t + 1) * ROWS, :]
    return total


def deriv_x(plan, matrix, pieces, lanes, energy=None):
    gx, rx, yc = plan.gx, plan.rx, plan.yc
    extra = 0 if energy is None else 1

    def kernel(high_ref, low_ref, *refs):
        ins, outs = refs[extra : extra + gx], refs[extra + gx :]
        high, low = high_ref[...], low_ref[...]
        for y in range(0, yc, 2):
            columns = [
                jnp.concatenate([p[pl.ds(y + k, rx, stride=yc), :] for p in ins], axis=0)
                for k in range(2)
            ]
            result = matrix_times(high, low, jnp.concatenate(columns, axis=1))
            for k in range(2):
                for t, out in enumerate(outs):
                    out[pl.ds(y + k, rx, stride=yc), :] = result[
                        t * rx : (t + 1) * rx, k * lanes : (k + 1) * lanes
                    ]
        if extra:
            for out in outs:
                out[rx * yc :, :] = refs[0][...]

    outs = [((rx + extra) * yc, lanes)] * gx
    ins = [*matrix] + ([energy] if extra else []) + list(pieces)
    return call(kernel, ins, outs)


def deriv_y(plan, matrix, pieces, lanes, with_energy=False):
    gy, sx, ry = plan.gy, plan.sx, plan.ry
    together = max(1, 2 * LANES // lanes)

    def kernel(high_ref, low_ref, *refs):
        ins, outs = refs[:gy], refs[gy : 2 * gy]
        high, low = high_ref[...], low_ref[...]
        for x in range(0, sx, together):
            columns = [
                jnp.concatenate([p[x + k] for p in ins], axis=0) for k in range(together)
            ]
            field = columns[0] if together == 1 else jnp.concatenate(columns, axis=1)
            result = matrix_times(high, low, field)
            for k in range(together):
                for t, out in enumerate(outs):
                    out[x + k] = result[t * ry : (t + 1) * ry, k * lanes : (k + 1) * lanes]
        if with_energy:
            energy_ref, ordered = refs[2 * gy :]
            energy_ref[...] = ordered_sum([p[sx, :ROWS, :] for p in ins], "gy", gy, ordered)

    outs, scratch = [(sx, ry, lanes)] * gy, []
    if with_energy:
        outs = outs + [(ROWS, lanes)]
        scratch = [pltpu.VMEM((gy * ROWS, lanes), jnp.float32)]
    return call(kernel, [*matrix, *pieces], outs, scratch)


def deriv_z(plan, matrix, field):
    rows = plan.rx * plan.ry
    block = rows // 4

    def kernel(high_ref, low_ref, f_ref, out_ref):
        for r in range(0, rows, block):
            part = slice(r, r + block)
            out_ref[part, :] = -times_matrix(f_ref[part, :], high_ref[...], low_ref[...])

    out = call(kernel, [*matrix, field.reshape(rows, plan.z)], [(rows, plan.z)])
    return out[0].reshape(field.shape)


def add_flux_z(plan, matrix, flux, chunk, lanes, terms):
    rows = plan.rx * plan.ry
    block = rows // 4
    flat = [a.reshape(rows, -1) for a in (flux, *terms)]

    def kernel(high_ref, low_ref, f_ref, *refs):
        own = slice(chunk * lanes, (chunk + 1) * lanes)
        for r in range(0, rows, block):
            part = slice(r, r + block)
            total = times_matrix(f_ref[part, :], high_ref[own, :], low_ref[own, :])
            if len(refs) > 1:
                rest = jnp.concatenate([t[part, :] for t in refs[1:-1]], axis=1)
                total = total + refs[0][part, :] + rest
            refs[-1][part, :] = total

    out = call(kernel, [*matrix, *flat], [(rows, plan.z)])
    return out[0].reshape(plan.rx, plan.ry, plan.z)


def pointwise(plan, density, grad_z, grad_y, grad_x, chunk, lanes, before):
    gx, gy, rx, ry, yc, sx = plan.gx, plan.gy, plan.rx, plan.ry, plan.yc, plan.sx
    extra = 0 if before is None else 1

    def kernel(*refs):
        n_ref, gz_ref = refs[0], refs[1]
        gy_refs = refs[2 : 2 + gy]
        gx_refs = refs[2 + gy : 2 + gy + gx]
        refs = refs[2 + gy + gx :]
        if extra:
            before_ref, refs = refs[0], refs[1:]
        fx_refs, fy_refs = refs[:gx], refs[gx : gx + gy]
        fz_ref, dd_ref, energy_ref = refs[gx + gy :]
        total = jnp.zeros((yc, lanes), jnp.float32)
        own = slice(chunk * lanes, (chunk + 1) * lanes)
        for part in range(gy):
            base = slot("gy", part, gy, sx)

            def step(inner, total, part=part, base=base):
                x = base + inner
                for t in range(gx):
                    rows = chunk_rows(plan, t)
                    n = n_ref[x, rows, own]
                    d_x = gx_refs[t][x]
                    d_y = gy_refs[part][inner, rows, own]
                    d_z = gz_ref[x, rows, own]
                    f, d_dens, d_grad = xc_partials(n, d_x * d_x + d_y * d_y + d_z * d_z)
                    twice = 2.0 * d_grad
                    fx_refs[t][x] = twice * d_x
                    fy_refs[part][inner, rows, :] = twice * d_y
                    fz_ref[x, rows, :] = twice * d_z
                    dd_ref[x, rows, :] = d_dens
                    total = total + f
                return total

            total = lax.fori_loop(0, sx, step, total)
        if extra:
            total = total + before_ref[...]
            for out in fy_refs:
                out[sx] = jnp.zeros((ry, lanes), jnp.float32)
                out[sx, :ROWS, :] = total
        energy_ref[...] = total

    ins = [density, grad_z, *grad_y, *[p.reshape(rx, yc, lanes) for p in grad_x]]
    if extra:
        ins.append(before)
    outs = [(rx, yc, lanes)] * gx + [(sx + extra, ry, lanes)] * gy
    outs += [(rx, ry, lanes)] * 2 + [(yc, lanes)]
    out = call(kernel, ins, outs, flops=1 << 32)
    flux_x = [p.reshape(rx * yc, lanes) for p in out[:gx]]
    return flux_x, out[gx : gx + gy], *out[gx + gy :]


def less_y(plan, base, div_y, lanes):
    gy, rx, ry, sx = plan.gy, plan.rx, plan.ry, plan.sx

    def kernel(base_ref, *refs):
        out_ref = refs[-1]
        for part in range(gy):
            rows = pl.ds(slot("gy", part, gy, sx), sx)
            for c in range(len(div_y)):
                where = slice(c * lanes, (c + 1) * lanes)
                out_ref[rows, :, where] = base_ref[rows, :, where] - refs[c * gy + part][...]

    ins = [base] + [p for pieces in div_y for p in pieces]
    return call(kernel, ins, [(rx, ry, plan.z)], flops=1 << 24)[0]


def finish(plan, base, div_x, chunk, lanes, before, scale):
    gx, rx, ry, yc = plan.gx, plan.rx, plan.ry, plan.yc
    last = scale is not None

    def kernel(base_ref, *refs):
        x_refs, refs = refs[:gx], refs[gx:]
        out_ref = refs[1] if last else refs[0]
        own = slice(chunk * lanes, (chunk + 1) * lanes)
        for t in range(gx):
            rows = chunk_rows(plan, t)
            out_ref[:, rows, :] = base_ref[:, rows, own] - x_refs[t][:rx]
        if last:
            energy_ref, ordered = refs[2:]
            total = ordered_sum([p[rx] for p in x_refs], "gx", gx, ordered)
            energy_ref[0, 0] = jnp.sum(total) * scale

    block = pl.BlockSpec((rx, ry, lanes), lambda s: (0, 0, chunk))
    ins = [base, *[p.reshape(-1, yc, lanes) for p in div_x]]
    specs = [VMEM] * len(ins)
    out_shape = [jax.ShapeDtypeStruct((rx, ry, plan.z), jnp.float32)]
    out_specs, scratch, aliases = [block], [], {}
    if last:
        aliases = {len(ins): 0}
        ins.append(before)
        specs.append(pl.BlockSpec(memory_space=pl.ANY))
        out_shape.append(jax.ShapeDtypeStruct((1, 1), jnp.float32))
        out_specs.append(pl.BlockSpec(memory_space=pltpu.SMEM))
        scratch = [pltpu.VMEM((gx * ROWS, lanes), jnp.float32)]
    return pl.pallas_call(
        kernel,
        grid=(1,),
        in_specs=specs,
        out_specs=out_specs,
        out_shape=out_shape,
        scratch_shapes=scratch,
        input_output_aliases=aliases,
        cost_estimate=pl.CostEstimate(flops=1 << 24, bytes_accessed=1 << 22, transcendentals=0),
        compiler_params=pltpu.CompilerParams(vmem_limit_bytes=GRANT),
        name="finish",
    )(*ins)


def body(density):
    return tiled_body(density)


def tiled_body(density):
    plan = Plan(density.shape)
    gx, gy = plan.gx, plan.gy
    count_x, count_y, count_z = plan.rx * gx, plan.ry * gy, plan.z
    matrix_x, matrix_y, matrix_z = split_matrix(count_x), split_matrix(count_y), split_matrix(count_z)
    lanes = plan.z // 2

    out = pack_x(plan, density, 0, lanes)
    dens_0 = rotate(out, "gx", gx)
    out = pack_y(plan, *after([density], out[0]))
    dens_y = rotate(out, "gy", gy)
    packed = pack_x(plan, *after([density], out[0]), 1, lanes)
    grad_z = deriv_z(plan, matrix_z, *after([density], packed[0]))
    dens_1 = rotate(after(packed, grad_z), "gx", gx)
    out_x = deriv_x(plan, matrix_x, after(dens_0, grad_z), lanes)
    grad_0 = rotate(out_x, "gx", gx)
    out = deriv_y(plan, matrix_y, after(dens_y, out_x[0]), plan.z)
    grad_y = rotate(out, "gy", gy)
    out_x = deriv_x(plan, matrix_x, after(dens_1, out[0]), lanes)
    grad_1 = rotate(out_x, "gx", gx)
    grad_0 = after(grad_0, out_x[0])
    f_x, f_y, f_z, part_0, energy = pointwise(plan, density, grad_z, grad_y, grad_0, 0, lanes, None)
    flux_0 = rotate(f_x, "gx", gx)
    flux_y = [rotate(f_y, "gy", gy)]
    base = add_flux_z(plan, matrix_z, *after([f_z], energy), 0, lanes, [])
    grad_1 = after(grad_1, base)
    f_x, f_y, f_z, part_1, energy = pointwise(
        plan, density, grad_z, grad_y, grad_1, 1, lanes, energy
    )
    flux_1 = rotate(f_x, "gx", gx)
    flux_y.append(rotate(f_y, "gy", gy))
    terms = [base, part_0, part_1]
    base = add_flux_z(plan, matrix_z, *after([f_z], energy), 1, lanes, terms)
    out_x = deriv_x(plan, matrix_x, after(flux_0, base), lanes)
    div_0 = rotate(out_x, "gx", gx)
    out = deriv_y(plan, matrix_y, after(flux_y[0], out_x[0]), lanes)
    div_y = [rotate(out, "gy", gy)]
    *out, energy = deriv_y(plan, matrix_y, after(flux_y[1], out[0]), lanes, True)
    div_y.append(rotate(out, "gy", gy))
    out_x = deriv_x(plan, matrix_x, after(flux_1, out[0]), lanes, energy)
    div_1 = rotate(out_x, "gx", gx)
    base = less_y(plan, *after([base], out_x[0]), div_y, lanes)
    scale = 1.0 / float(count_x * count_y * count_z)
    (half,) = finish(plan, base, div_0, 0, lanes, None, None)
    done, energy = finish(plan, base, div_1, 1, lanes, half, scale)
    return done, energy[0, 0]


def xc_energy(electrons, grad_sq):
    k_fermi = jnp.cbrt(3.0 * math.pi**2 * electrons)
    exch_unif = -0.75 * k_fermi / math.pi
    s_square = grad_sq / (4.0 * k_fermi**2 * electrons**2)
    enhance = 1.0 + pbe_kappa - pbe_kappa / (1.0 + pbe_mu * s_square / pbe_kappa)
    wigner = jnp.cbrt(3.0 / (4.0 * math.pi * electrons))
    root_rs = jnp.sqrt(wigner)
    series = (
        2.0
        * pw_coef
        * (
            pw_first * root_rs
            + pw_second * wigner
            + pw_third * wigner * root_rs
            + pw_fourth * wigner**2
        )
    )
    corr_unif = -2.0 * pw_coef * (1.0 + pw_alpha * wigner) * jnp.log(1.0 + 1.0 / series)
    screen_sq = 4.0 * k_fermi / math.pi
    t_square = grad_sq / (4.0 * screen_sq * electrons**2)
    factor = pbe_beta / pbe_gamma / jnp.expm1(-corr_unif / pbe_gamma)
    scaled = factor * t_square
    gradient_term = pbe_gamma * jnp.log(
        1.0 + pbe_beta / pbe_gamma * t_square * (1.0 + scaled) / (1.0 + scaled + scaled**2)
    )
    return electrons * (exch_unif * enhance + corr_unif + gradient_term)


def summed_energy(electrons, grad_sq):
    return jnp.sum(xc_energy(electrons, grad_sq))


def total_energy(energy_local, cells):
    return lax.psum(energy_local, ("gx", "gy")) / float(cells)


def wavenum(index, count):
    signed = jnp.where(index < count // 2, index, index - count)
    signed = jnp.where(index == count // 2, 0, signed)
    return signed.astype(jnp.float32) * (2.0 * math.pi / (count * spacing))


def dft_tables(count, order):
    columns = jnp.arange(count, dtype=jnp.int32)
    phase = (order[:, None] * columns[None, :] % count).astype(jnp.float32) * (
        2.0 * math.pi / count
    )
    return (jnp.cos(phase), jnp.sin(phase))


def plain_matrix(count):
    positions = jnp.arange(count, dtype=jnp.int32)
    cosine, sine = dft_tables(count, positions)
    waves = wavenum(positions, count)
    first = jnp.dot(cosine.T * waves[None, :], sine, precision=lax.Precision.HIGHEST)
    second = jnp.dot(sine.T * waves[None, :], cosine, precision=lax.Precision.HIGHEST)
    return (first - second) / float(count)


def plain_body(density):
    count_gx = lax.axis_size("gx")
    count_gy = lax.axis_size("gy")
    rows_x, rows_y, count_z = density.shape
    count_x = rows_x * count_gx
    count_y = rows_y * count_gy
    deriv_x = plain_matrix(count_x)
    deriv_y = plain_matrix(count_y)
    deriv_z = plain_matrix(count_z)

    def line_x(piece):
        flat = piece.reshape(piece.shape[0], piece.shape[1] * piece.shape[2])
        result = jnp.dot(deriv_x, flat, precision=lax.Precision.HIGHEST)
        return result.reshape(piece.shape)

    def line_y(piece):
        turned = jnp.swapaxes(piece, 0, 1)
        flat = turned.reshape(turned.shape[0], turned.shape[1] * turned.shape[2])
        result = jnp.dot(deriv_y, flat, precision=lax.Precision.HIGHEST).reshape(turned.shape)
        return jnp.swapaxes(result, 0, 1)

    def along_x(field):
        lines = line_x(lax.all_to_all(field, "gx", split_axis=2, concat_axis=0, tiled=True))
        return lax.all_to_all(lines, "gx", split_axis=0, concat_axis=2, tiled=True)

    def along_y(field):
        lines = line_y(lax.all_to_all(field, "gy", split_axis=2, concat_axis=1, tiled=True))
        return lax.all_to_all(lines, "gy", split_axis=1, concat_axis=2, tiled=True)

    def along_z(field):
        flat = field.reshape(field.shape[0] * field.shape[1], field.shape[2])
        result = jnp.dot(flat, deriv_z.T, precision=lax.Precision.HIGHEST)
        return result.reshape(field.shape)

    gradients = [along_x(density), along_y(density), along_z(density)]
    grad_sq = (
        gradients[0] * gradients[0] + gradients[1] * gradients[1] + gradients[2] * gradients[2]
    )
    energy_local, partials = jax.value_and_grad(summed_energy, argnums=(0, 1))(density, grad_sq)
    d_dens, d_grad = partials
    fluxes = [2.0 * d_grad * gradient for gradient in gradients]
    divergence = along_x(fluxes[0]) + along_y(fluxes[1]) + along_z(fluxes[2])
    potential = d_dens - divergence
    return (potential, total_energy(energy_local, count_x * count_y * count_z))


def solution(mesh):
    in_specs = (P("gx", "gy", None),)
    out_specs = (P("gx", "gy", None), P())

    def run(density):
        gx, gy = mesh.shape["gx"], mesh.shape["gy"]
        x, y, z = density.shape
        tiled = Plan.fits((x // gx, y // gy, z), gx, gy)
        step = jax.shard_map(
            body if tiled else plain_body,
            mesh=mesh,
            in_specs=in_specs,
            out_specs=out_specs,
            check_vma=False,
        )
        return step(density)

    return run
```

```python
import math

import jax
import jax.numpy as jnp
import numpy as np
from jax import lax
from jax.experimental import pallas as pl
from jax.experimental.pallas import tpu as pltpu
from jax.sharding import PartitionSpec as P


spacing = 1.0
pbe_kappa = 0.804
pbe_mu = 0.2195149727645171
pbe_beta = 0.06672455060314922
pbe_gamma = 0.031090690869654894
pw_coef = 0.0310907
pw_alpha = 0.2137
pw_first = 7.5957
pw_second = 3.5876
pw_third = 1.6382
pw_fourth = 0.49294

GRANT = 16 << 20
LANES = 128
CHUNKS = 4
CHIPS = 4
ROWS = 8


def deriv_matrix(count):
    index = np.arange(count)
    signed = np.where(index < count // 2, index, index - count)
    signed = np.where(index == count // 2, 0, signed)
    waves = signed * (2.0 * math.pi / (count * spacing))
    return np.fft.ifft(1j * waves[:, None] * np.fft.fft(np.eye(count), axis=0), axis=0).real


def split_matrix(count):
    return split_values(deriv_matrix(count))


def split_values(matrix):
    high = matrix.astype(jnp.bfloat16)
    low = (matrix - high.astype(np.float64)).astype(jnp.bfloat16)
    return jnp.asarray(high), jnp.asarray(low)


def halves(field):
    high = field.astype(jnp.bfloat16)
    return high, (field - high.astype(jnp.float32)).astype(jnp.bfloat16)


def dot(left, right):
    return jnp.dot(left, right, preferred_element_type=jnp.float32)


def matrix_times(high, low, field):
    f_high, f_low = halves(field)
    return dot(high, f_high) + (dot(high, f_low) + dot(low, f_high))


def times_matrix(field, high, low):
    f_high, f_low = halves(field)
    return dot(f_high, high) + (dot(f_low, high) + dot(f_high, low))


def xc_partials(n, g):
    c_fermi = (3.0 * math.pi**2) ** (1.0 / 3.0)
    c_wigner = (3.0 / (4.0 * math.pi)) ** (1.0 / 3.0)
    c_ratio = pbe_beta / pbe_gamma
    v = jnp.exp(jnp.log(n) * (-1.0 / 6.0))
    v2 = v * v
    v4 = v2 * v2
    n13 = n * v4
    v8 = v4 * v4
    v14 = v8 * v4 * v2
    ex = n13 * (-0.75 * c_fermi / math.pi)
    s_scale = (v14 * v2) * (1.0 / (4.0 * c_fermi**2))
    s2 = g * s_scale
    r_x = 1.0 / (pbe_kappa + pbe_mu * s2)
    fx = (1.0 + pbe_kappa) - pbe_kappa**2 * r_x
    dfx = (pbe_mu * pbe_kappa**2) * (r_x * r_x)
    rs = c_wigner * v2
    root = math.sqrt(c_wigner) * v
    q_series = (2.0 * pw_coef) * (
        root * (pw_first + pw_third * rs) + rs * (pw_second + pw_fourth * rs)
    )
    q_slope = (2.0 * pw_coef) * (
        root * (0.5 * pw_first + 1.5 * pw_third * rs) + rs * (pw_second + (2.0 * pw_fourth) * rs)
    )
    r_q = 1.0 / (q_series * (q_series + 1.0))
    log_q = jnp.log(1.0 + (q_series + 1.0) * r_q)
    lead = (2.0 * pw_coef) * (1.0 + pw_alpha * rs)
    ec = -lead * log_q
    nd = (-1.0 / 3.0) * (lead * q_slope * r_q - (2.0 * pw_coef * pw_alpha) * rs * log_q)
    t_scale = v14 * (math.pi / (16.0 * c_fermi))
    t2 = g * t_scale
    grown = jnp.exp(ec * (-1.0 / pbe_gamma))
    r_e = 1.0 / (grown - 1.0)
    factor = c_ratio * r_e
    q = factor * t2
    den = 1.0 + q + q * q
    full = den + c_ratio * t2 * (1.0 + q)
    r_d = 1.0 / (den * full)
    h = pbe_gamma * jnp.log(full * full * r_d)
    h_t = pbe_beta * (1.0 + 2.0 * q) * r_d
    h_p = (-pbe_beta) * (t2 * t2) * (q * (2.0 + q)) * r_d
    energy = n * (ex * fx + ec + h)
    d_grad = n * (ex * dfx * s_scale + h_t * t_scale)
    d_dens = (
        ex * ((4.0 / 3.0) * fx - (8.0 / 3.0) * (s2 * dfx))
        + ec
        + h
        + nd * (1.0 + h_p * factor * grown * r_e * (1.0 / pbe_gamma))
        - (7.0 / 3.0) * t2 * h_t
    )
    return energy, d_dens, d_grad


def slot(axis, step, size, width):
    return pl.multiple_of(lax.rem(lax.axis_index(axis) + step, size) * width, width)


VMEM = pl.BlockSpec(memory_space=pltpu.VMEM)
HBM = pl.BlockSpec(memory_space=pltpu.HBM)


def call(kernel, ins, outs, scratch=(), flops=1 << 28):
    return pl.pallas_call(
        kernel,
        in_specs=[VMEM] * len(ins),
        out_specs=[VMEM] * len(outs),
        out_shape=[jax.ShapeDtypeStruct(o, jnp.float32) for o in outs],
        scratch_shapes=list(scratch),
        cost_estimate=pl.CostEstimate(
            flops=flops,
            bytes_accessed=sum(4 * math.prod(o) for o in outs) + sum(4 * a.size for a in ins),
            transcendentals=0,
        ),
        compiler_params=pltpu.CompilerParams(vmem_limit_bytes=GRANT),
    )(*ins)


def after(arrays, token):
    return lax.optimization_barrier((list(arrays), token))[0]


class Plan:
    def __init__(self, shape):
        self.gx, self.gy = lax.axis_size("gx"), lax.axis_size("gy")
        self.own, self.ry, self.z = shape
        self.rows = 2 * self.own
        self.half = self.z // 2
        self.yc = self.ry // CHUNKS
        self.sx = self.rows // self.gy

    @staticmethod
    def fits(shape, gx, gy):
        rx, ry, z = shape
        return (
            gx == 2 * CHIPS
            and z == 2 * LANES
            and ry % (CHUNKS * ROWS) == 0
            and 2 * rx % (4 * gy) == 0
            and rx % ROWS == 0
        )


def pairs(chips):
    return [(2 * a + k, 2 * b + k) for a, b in chips for k in range(2)]


INWARD = pairs([(0, 1), (3, 2)])
ACROSS = pairs([(1, 2), (2, 1)])
OUTWARD = pairs([(1, 0), (2, 3)])
NEAR = pairs([(0, 1), (1, 0), (2, 3), (3, 2)])
FAR = pairs([(0, 3), (3, 0), (1, 2), (2, 1)])
SWAP = [(i, i ^ 1) for i in range(2 * CHIPS)]


def move(array, to):
    return lax.ppermute(array, "gx", to)


def core():
    return lax.rem(lax.axis_index("gx"), 2)


def chip():
    return lax.div(lax.axis_index("gx"), 2)


def is_inner():
    return jnp.logical_or(chip() == 1, chip() == 2)


def at_core(k, width):
    return pl.ds(pl.multiple_of(k * width, width), width)


def assemble(plan, density, far):
    def kernel(own_ref, far_ref, *refs):
        outs, semaphore = refs[:-1], refs[-1]
        copies = []
        for h in range(2):
            k = core() if h == 0 else 1 - core()
            lanes = at_core(k, plan.half)
            for c in range(CHUNKS):
                part = (slice(None), pl.ds(c * plan.yc, plan.yc), lanes)
                out = outs[h * CHUNKS + c]
                for j, (ref, place) in enumerate(((own_ref, core()), (far_ref, 1 - core()))):
                    target = out.at[at_core(place, plan.own)]
                    sem = semaphore.at[(h * CHUNKS + c) * 2 + j]
                    copies.append(pltpu.make_async_copy(ref.at[part], target, sem))
        for copy in copies:
            copy.start()
        for copy in copies:
            copy.wait()

    shape = jax.ShapeDtypeStruct((plan.rows, plan.yc, plan.half), jnp.float32)
    out = pl.pallas_call(
        kernel,
        in_specs=[pl.BlockSpec(memory_space=pl.ANY)] * 2,
        out_specs=[VMEM] * (2 * CHUNKS),
        out_shape=[shape] * (2 * CHUNKS),
        scratch_shapes=[pltpu.SemaphoreType.DMA((4 * CHUNKS,))],
        cost_estimate=pl.CostEstimate(flops=1 << 20, bytes_accessed=1 << 22, transcendentals=0),
        compiler_params=pltpu.CompilerParams(vmem_limit_bytes=GRANT),
        name="assemble",
    )(density, far)
    return out


def pack_y(plan, chunks, stacked=False):
    def kernel(*refs):
        ins, outs = refs[:CHUNKS], refs[CHUNKS:]
        for t, out in enumerate(outs[: plan.gy]):
            for c, ref in enumerate(ins):
                rows = pl.ds(slot("gy", t, plan.gy, plan.sx), plan.sx)
                out[:, c * plan.yc : (c + 1) * plan.yc, :] = ref[rows]
        if stacked:
            for c, ref in enumerate(ins):
                outs[-1][c] = ref[...]

    outs = [(plan.sx, plan.ry, plan.half)] * plan.gy
    if stacked:
        outs = outs + [(CHUNKS, plan.rows, plan.yc, plan.half)]
    return call(kernel, chunks, outs, flops=1 << 20)


def join_y(plan, pieces):
    parts = CHUNKS - 1

    def kernel(*refs):
        ins, outs = refs[: plan.gy * parts], refs[plan.gy * parts :]
        for t, out in enumerate(outs):
            for c in range(parts):
                out[:, c * plan.yc : (c + 1) * plan.yc, :] = ins[t * parts + c][...]

    outs = [(plan.sx, parts * plan.yc, plan.half)] * plan.gy
    return call(kernel, pieces, outs, flops=1 << 20)


def add(tiles):
    def kernel(a_ref, b_ref, out_ref):
        out_ref[...] = a_ref[...] + b_ref[...]

    return call(kernel, tiles, [tiles[0].shape], flops=1 << 10)


def stack(plan, chunks):
    def kernel(*refs):
        for c in range(CHUNKS):
            refs[-1][c] = refs[c][...]

    outs = [(CHUNKS, plan.rows, plan.yc, plan.half)]
    return call(kernel, chunks, outs, flops=1 << 20)


def rotate(pieces, axis, size):
    arrived = [pieces[0]] + [None] * (size - 1)
    for t in sorted(range(1, size), key=lambda t: abs(2 * t - size)):
        to = [(i, (i + t) % size) for i in range(size)]
        arrived[size - t] = lax.ppermute(pieces[t], axis, to)
    return arrived


def ordered_sum(pieces, axis, size, scratch):
    for t, piece in enumerate(pieces):
        scratch[pl.ds(slot(axis, t, size, ROWS), ROWS), :] = piece
    total = scratch[:ROWS, :]
    for t in range(1, size):
        total = total + scratch[t * ROWS : (t + 1) * ROWS, :]
    return total


def deriv_x(plan, matrix, pieces, count):
    rows, yc, lanes = plan.rows, plan.yc, plan.half

    def kernel(high_ref, low_ref, *refs):
        ins, outs = refs[:CHIPS], refs[CHIPS:]
        size = CHIPS * rows
        first = pl.multiple_of(lax.div(chip(), CHIPS // 2) * size, size)
        high = high_ref[pl.ds(first, count * rows), :]
        low = low_ref[pl.ds(first, count * rows), :]
        for y in range(0, yc, 2):
            columns = [
                jnp.concatenate([p[pl.ds(y + k, rows, stride=yc), :] for p in ins], axis=0)
                for k in range(2)
            ]
            result = matrix_times(high, low, jnp.concatenate(columns, axis=1))
            for k in range(2):
                for t, out in enumerate(outs):
                    out[pl.ds(y + k, rows, stride=yc), :] = result[
                        t * rows : (t + 1) * rows, k * lanes : (k + 1) * lanes
                    ]

    flat = [p.reshape(rows * yc, lanes) for p in pieces]
    out = call(kernel, [*flat[:0], *matrix, *flat], [(rows * yc, lanes)] * count)
    return [o.reshape(rows, yc, lanes) for o in out]


def deriv_y(plan, matrix, pieces, with_energy=False):
    gy, sx, ry, lanes = plan.gy, plan.sx, plan.ry, plan.half
    parts = len(pieces[0])

    def kernel(high_ref, low_ref, *refs):
        ins, outs = refs[: gy * parts], refs[gy * parts : gy * parts + gy]
        high, low = high_ref[...], low_ref[...]

        def step(group, carry):
            for x in (4 * group, 4 * group + 2):
                columns = [jnp.concatenate([p[x + k] for p in ins], axis=0) for k in range(2)]
                result = matrix_times(high, low, jnp.concatenate(columns, axis=1))
                for k in range(2):
                    for t, out in enumerate(outs):
                        out[x + k] = result[t * ry : (t + 1) * ry, k * lanes : (k + 1) * lanes]
            return carry

        lax.fori_loop(0, sx // 4, step, 0)
        if with_energy:
            energy_ref, ordered = refs[gy * parts + gy :]
            tiles = [ins[t * parts + parts - 1][sx, :ROWS, :] for t in range(gy)]
            energy_ref[...] = ordered_sum(tiles, "gy", gy, ordered)

    outs, scratch = [(sx, ry, lanes)] * gy, []
    if with_energy:
        outs = outs + [(ROWS, lanes)]
        scratch = [pltpu.VMEM((gy * ROWS, lanes), jnp.float32)]
    return call(kernel, [*matrix, *[c for p in pieces for c in p]], outs, scratch)


def deriv_z(plan, matrix, chunks, others, terms=None):
    rows, lanes, count = plan.rows * plan.yc, plan.half, len(chunks)
    stacked = len(others) == 1
    given = count + len(others)

    def kernel(high_ref, low_ref, *refs):
        outs = refs[-count:]
        for c in range(count):
            other = refs[count][c] if stacked else refs[count + c][...]
            field = jnp.concatenate([refs[c][...], other], axis=1)
            result = -times_matrix(field, high_ref[:, :lanes], low_ref[:, :lanes])
            outs[c][...] = result if terms is None else refs[given + c][...] - result

    ins = [a.reshape(rows, lanes) for a in chunks]
    ins += [a.reshape(*a.shape[: a.ndim - 3], rows, lanes) for a in others]
    ins += [a.reshape(rows, lanes) for a in terms or []]
    out = call(kernel, [*matrix, *ins], [(rows, lanes)] * count)
    return [o.reshape(plan.rows, plan.yc, lanes) for o in out]


def pointwise(plan, chunk, dens, grad_z, grad_y, grad_x, mirror, before):
    gy, rows, yc, sx, lanes = plan.gy, plan.rows, plan.yc, plan.sx, plan.half
    last = chunk == CHUNKS - 1
    extra = 1 if last else 0
    ins = [dens, grad_z, *grad_y, *grad_x] + ([] if before is None else [before])

    def kernel(*refs):
        n_ref, gz_ref = refs[:2]
        gy_refs = refs[2 : 2 + gy]
        gx_refs = refs[2 + gy : 2 + gy + len(grad_x)]
        outs = refs[len(ins) :]
        fx_ref = outs[0]
        if not mirror:
            fy_refs, (fz_ref, dd_ref, energy_ref) = outs[1 : 1 + gy], outs[1 + gy :]
            inner_chip = is_inner()
        total = jnp.zeros((ROWS, lanes), jnp.float32)

        def step(inner, total):
            for part in range(gy):
                x = slot("gy", part, gy, sx) + inner
                for y in range(0, yc, ROWS):
                    local = pl.ds(y, ROWS)
                    n = n_ref[x, local, :]
                    d_x = gx_refs[0][x, local, :]
                    if not mirror:
                        d_x = jnp.where(inner_chip, d_x, gx_refs[1][x, local, :])
                    d_y = gy_refs[part][inner, pl.ds(chunk * yc + y, ROWS), :]
                    d_z = gz_ref[x, local, :]
                    f, d_dens, d_grad = xc_partials(n, d_x * d_x + d_y * d_y + d_z * d_z)
                    twice = 2.0 * d_grad
                    fx_ref[x, local, :] = twice * d_x
                    if not mirror:
                        fy_refs[part][inner, local, :] = twice * d_y
                        fz_ref[x, local, :] = twice * d_z
                        dd_ref[x, local, :] = d_dens
                        total = total + f
            return total

        total = lax.fori_loop(0, sx, step, total)
        if not mirror:
            if before is not None:
                total = total + refs[len(ins) - 1][...]
            if last:
                for out in fy_refs:
                    out[sx] = jnp.zeros((yc, lanes), jnp.float32)
                    out[sx, :ROWS, :] = total
            energy_ref[...] = total

    block = (rows, yc, lanes)
    outs = [block]
    if not mirror:
        outs += [(sx + extra, yc, lanes)] * gy + [block] * 2 + [(ROWS, lanes)]
    return call(kernel, ins, outs, flops=1 << 30)


def finish(plan, chunk, base, div_y, div_x):
    gy, rows, yc, sx, lanes, own = plan.gy, plan.rows, plan.yc, plan.sx, plan.half, plan.own

    def kernel(base_ref, *refs):
        y_refs, (inner_ref, outer_ref, keep_ref, give_ref, full) = refs[:gy], refs[gy:]
        own_y = slice(chunk * yc, (chunk + 1) * yc)
        inner_chip = is_inner()
        for t in range(gy):
            part = pl.ds(slot("gy", t, gy, sx), sx)
            d_x = jnp.where(inner_chip, inner_ref[part], outer_ref[part])
            full[part] = base_ref[part] - (d_x + y_refs[t][:, own_y, :])
        keep_ref[...] = full[at_core(core(), own)]
        give_ref[...] = full[at_core(1 - core(), own)]

    scratch = [pltpu.VMEM((rows, yc, lanes), jnp.float32)]
    ins = [base, *div_y, *div_x]
    return call(kernel, ins, [(own, yc, lanes)] * 2, scratch, flops=1 << 24)


def place(plan, kept, given, energies, scale):
    yc, half = plan.yc, plan.half
    count = 2 * CHUNKS

    def kernel(*refs):
        ins, tiles = refs[:count], refs[count : count + 2]
        out_ref, energy_ref, semaphore = refs[count + 2 :]
        copies = []
        for j, ref in enumerate(ins):
            c, k = j % CHUNKS, core() if j < CHUNKS else 1 - core()
            target = out_ref.at[:, pl.ds(c * yc, yc), at_core(k, half)]
            copies.append(pltpu.make_async_copy(ref, target, semaphore.at[j]))
        for copy in copies:
            copy.start()
        energy_ref[0, 0] = jnp.sum(tiles[0][...] + tiles[1][...]) * scale
        for copy in copies:
            copy.wait()

    return pl.pallas_call(
        kernel,
        in_specs=[VMEM] * (count + 2),
        out_specs=[pl.BlockSpec(memory_space=pl.ANY), pl.BlockSpec(memory_space=pltpu.SMEM)],
        out_shape=[
            jax.ShapeDtypeStruct((plan.own, plan.ry, plan.z), jnp.float32),
            jax.ShapeDtypeStruct((1, 1), jnp.float32),
        ],
        scratch_shapes=[pltpu.SemaphoreType.DMA((count,))],
        cost_estimate=pl.CostEstimate(flops=1 << 20, bytes_accessed=1 << 22, transcendentals=0),
        compiler_params=pltpu.CompilerParams(vmem_limit_bytes=GRANT),
        name="place",
    )(*kept, *given, *energies)


def body(density):
    return tiled_body(density)


def inner_matrices(plan):
    matrix = deriv_matrix(plan.own * plan.gx)
    found = []
    for order in ((1, 0, 2, 3), (2, 3, 1, 0)):
        index = np.concatenate([np.arange(plan.rows) + plan.rows * o for o in order])
        found.append(matrix[index][:, index])
    return split_values(np.concatenate(found))


def tiled_body(density):
    plan = Plan(density.shape)
    gx, gy = plan.gx, plan.gy
    matrix_x = inner_matrices(plan)
    matrix_y, matrix_z = split_matrix(plan.ry * gy), split_matrix(plan.z)
    token = None
    chunks = range(CHUNKS)

    def run(kernel, arrays, *args, **kwargs):
        nonlocal token
        if token is not None:
            arrays = after(arrays, token)
        out = kernel(arrays, *args, **kwargs)
        token = out[0]
        return out

    far = move(density, SWAP)
    out = run(lambda a: assemble(plan, *a), [density, far])
    dens, other = out[:CHUNKS], out[CHUNKS:]
    mirror, outer, beyond = [], [], []
    for c in chunks:
        mirror.append(move(dens[c], ACROSS))
        outer.append(move(dens[c], INWARD))
    out = run(lambda a: pack_y(plan, a), dens)
    dens_y = rotate(out, "gy", gy)
    grad_z, early = [], CHUNKS // 2
    for part in (chunks[:early], chunks[early:]):
        arrays = [dens[c] for c in part] + [other[c] for c in part]
        grad_z += run(lambda a: deriv_z(plan, matrix_z, a[: len(a) // 2], a[len(a) // 2 :]), arrays)
    beyond = [move(outer[c], ACROSS) for c in chunks]
    out = run(lambda a: deriv_y(plan, matrix_y, [[p] for p in a]), dens_y)
    grad_y = rotate(out, "gy", gy)
    grad_x, flux, relay, mirror_f, div_x = {}, {}, {}, {}, {}

    def gradient_x(c):
        pieces = [dens[c], outer[c], mirror[c], beyond[c]]
        own, out_, mirrored = run(lambda a: deriv_x(plan, matrix_x, a, 3), pieces)
        return (own, move(out_, OUTWARD)), mirrored

    grad_x[0] = gradient_x(0)

    energy = None

    def point(c):
        nonlocal energy
        arrays = [dens[c], grad_z[c], *grad_y, *grad_x[c][0]]
        f_x, *out = run(
            lambda a: pointwise(
                plan, c, a[0], a[1], a[2 : 2 + gy], a[2 + gy :], False, energy
            ),
            arrays,
        )
        energy = out[-1]
        f_z, part = out[gy], out[gy + 1]
        inward = move(f_x, INWARD)
        return dict(x=f_x, outer=inward, y=out[:gy], z=f_z, d=part)

    def mirrored_point(c):
        arrays = [mirror[c], mirror_gz[c], *mirror_gy, grad_x[c][1]]
        return run(
            lambda a: pointwise(plan, c, a[0], a[1], a[2 : 2 + gy], a[2 + gy :], True, None), arrays
        )[0]

    def relay_on(c):
        relay[c] = move(flux[c]["outer"], ACROSS)

    def divergence_x(c):
        pieces = [flux[c]["x"], flux[c]["outer"], mirror_f[c], relay[c]]
        own, out_ = run(lambda a: deriv_x(plan, matrix_x, a, 2), pieces)
        div_x[c] = own, move(out_, OUTWARD)

    flux[0] = point(0)
    *out, both = run(lambda a: pack_y(plan, a, True), mirror)
    mirror_y = rotate(out, "gy", gy)
    mirror_other = move(both, SWAP)
    grad_x[1] = gradient_x(1)
    mirror_gz = run(
        lambda a: deriv_z(plan, matrix_z, a[:CHUNKS], a[CHUNKS:]), [*mirror, mirror_other]
    )
    grad_x[2] = gradient_x(2)
    flux[1] = point(1)
    relay_on(0)
    out = run(lambda a: deriv_y(plan, matrix_y, [[p] for p in a]), mirror_y)
    mirror_gy = rotate(out, "gy", gy)
    grad_x[3] = gradient_x(3)
    flux[2] = point(2)
    relay_on(1)
    flat = [flux[c]["y"][t] for t in range(gy) for c in chunks[:-1]]
    early = rotate(run(lambda a: join_y(plan, a), flat), "gy", gy)
    flux[3] = point(3)
    relay_on(2)
    mirror_f[0] = mirrored_point(0)
    divergence_x(0)
    mirror_f[1] = mirrored_point(1)
    divergence_x(1)
    relay_on(3)
    mirror_f[2] = mirrored_point(2)
    late = rotate(flux[CHUNKS - 1]["y"], "gy", gy)
    flat = [p for pair in zip(early, late) for p in pair]
    *out, energy = run(
        lambda a: deriv_y(plan, matrix_y, [a[2 * t : 2 * t + 2] for t in range(gy)], True), flat
    )
    div_y = rotate(out, "gy", gy)
    tiles = [energy, move(energy, SWAP)]
    divergence_x(2)
    (both,) = run(lambda a: stack(plan, a), [flux[c]["z"] for c in chunks])
    flux_other = move(both, SWAP)
    mirror_f[3] = mirrored_point(3)
    (energy,) = run(add, tiles)
    tiles = [energy, move(energy, NEAR)]
    divergence_x(3)
    base = run(
        lambda a: deriv_z(plan, matrix_z, a[:CHUNKS], a[CHUNKS : CHUNKS + 1], a[CHUNKS + 1 :]),
        [flux[c]["z"] for c in chunks] + [flux_other] + [flux[c]["d"] for c in chunks],
    )
    (energy,) = run(add, tiles)
    tiles = [energy, move(energy, FAR)]
    kept, given = [], []
    for c in chunks:
        keep, give = run(
            lambda a, c=c: finish(plan, c, a[0], a[1 : 1 + gy], a[1 + gy :]),
            [base[c], *div_y, *div_x[c]],
        )
        kept.append(keep)
        given.append(move(give, SWAP))
    scale = 1.0 / float(plan.own * gx * plan.ry * gy * plan.z)
    done, energy = run(
        lambda a: place(plan, a[:CHUNKS], a[CHUNKS : 2 * CHUNKS], a[2 * CHUNKS :], scale),
        [*kept, *given, *tiles],
    )
    return done, energy[0, 0]


def xc_energy(electrons, grad_sq):
    k_fermi = jnp.cbrt(3.0 * math.pi**2 * electrons)
    exch_unif = -0.75 * k_fermi / math.pi
    s_square = grad_sq / (4.0 * k_fermi**2 * electrons**2)
    enhance = 1.0 + pbe_kappa - pbe_kappa / (1.0 + pbe_mu * s_square / pbe_kappa)
    wigner = jnp.cbrt(3.0 / (4.0 * math.pi * electrons))
    root_rs = jnp.sqrt(wigner)
    series = (
        2.0
        * pw_coef
        * (
            pw_first * root_rs
            + pw_second * wigner
            + pw_third * wigner * root_rs
            + pw_fourth * wigner**2
        )
    )
    corr_unif = -2.0 * pw_coef * (1.0 + pw_alpha * wigner) * jnp.log(1.0 + 1.0 / series)
    screen_sq = 4.0 * k_fermi / math.pi
    t_square = grad_sq / (4.0 * screen_sq * electrons**2)
    factor = pbe_beta / pbe_gamma / jnp.expm1(-corr_unif / pbe_gamma)
    scaled = factor * t_square
    gradient_term = pbe_gamma * jnp.log(
        1.0 + pbe_beta / pbe_gamma * t_square * (1.0 + scaled) / (1.0 + scaled + scaled**2)
    )
    return electrons * (exch_unif * enhance + corr_unif + gradient_term)


def summed_energy(electrons, grad_sq):
    return jnp.sum(xc_energy(electrons, grad_sq))


def total_energy(energy_local, cells):
    return lax.psum(energy_local, ("gx", "gy")) / float(cells)


def wavenum(index, count):
    signed = jnp.where(index < count // 2, index, index - count)
    signed = jnp.where(index == count // 2, 0, signed)
    return signed.astype(jnp.float32) * (2.0 * math.pi / (count * spacing))


def dft_tables(count, order):
    columns = jnp.arange(count, dtype=jnp.int32)
    phase = (order[:, None] * columns[None, :] % count).astype(jnp.float32) * (
        2.0 * math.pi / count
    )
    return (jnp.cos(phase), jnp.sin(phase))


def plain_matrix(count):
    positions = jnp.arange(count, dtype=jnp.int32)
    cosine, sine = dft_tables(count, positions)
    waves = wavenum(positions, count)
    first = jnp.dot(cosine.T * waves[None, :], sine, precision=lax.Precision.HIGHEST)
    second = jnp.dot(sine.T * waves[None, :], cosine, precision=lax.Precision.HIGHEST)
    return (first - second) / float(count)


def plain_body(density):
    count_gx = lax.axis_size("gx")
    count_gy = lax.axis_size("gy")
    rows_x, rows_y, count_z = density.shape
    count_x = rows_x * count_gx
    count_y = rows_y * count_gy
    deriv_x = plain_matrix(count_x)
    deriv_y = plain_matrix(count_y)
    deriv_z = plain_matrix(count_z)

    def line_x(piece):
        flat = piece.reshape(piece.shape[0], piece.shape[1] * piece.shape[2])
        result = jnp.dot(deriv_x, flat, precision=lax.Precision.HIGHEST)
        return result.reshape(piece.shape)

    def line_y(piece):
        turned = jnp.swapaxes(piece, 0, 1)
        flat = turned.reshape(turned.shape[0], turned.shape[1] * turned.shape[2])
        result = jnp.dot(deriv_y, flat, precision=lax.Precision.HIGHEST).reshape(turned.shape)
        return jnp.swapaxes(result, 0, 1)

    def along_x(field):
        lines = line_x(lax.all_to_all(field, "gx", split_axis=2, concat_axis=0, tiled=True))
        return lax.all_to_all(lines, "gx", split_axis=0, concat_axis=2, tiled=True)

    def along_y(field):
        lines = line_y(lax.all_to_all(field, "gy", split_axis=2, concat_axis=1, tiled=True))
        return lax.all_to_all(lines, "gy", split_axis=1, concat_axis=2, tiled=True)

    def along_z(field):
        flat = field.reshape(field.shape[0] * field.shape[1], field.shape[2])
        result = jnp.dot(flat, deriv_z.T, precision=lax.Precision.HIGHEST)
        return result.reshape(field.shape)

    gradients = [along_x(density), along_y(density), along_z(density)]
    grad_sq = (
        gradients[0] * gradients[0] + gradients[1] * gradients[1] + gradients[2] * gradients[2]
    )
    energy_local, partials = jax.value_and_grad(summed_energy, argnums=(0, 1))(density, grad_sq)
    d_dens, d_grad = partials
    fluxes = [2.0 * d_grad * gradient for gradient in gradients]
    divergence = along_x(fluxes[0]) + along_y(fluxes[1]) + along_z(fluxes[2])
    potential = d_dens - divergence
    return (potential, total_energy(energy_local, count_x * count_y * count_z))


def solution(mesh):
    in_specs = (P("gx", "gy", None),)
    out_specs = (P("gx", "gy", None), P())

    def run(density):
        gx, gy = mesh.shape["gx"], mesh.shape["gy"]
        x, y, z = density.shape
        tiled = Plan.fits((x // gx, y // gy, z), gx, gy)
        step = jax.shard_map(
            body if tiled else plain_body,
            mesh=mesh,
            in_specs=in_specs,
            out_specs=out_specs,
            check_vma=False,
        )
        return step(density)

    return run
```
